512 devices in a mesh: gy: 32 (over z, y_lo), gz: 16 (over x, y_hi, core).
Axes of the slice: x: 4, y: 8 (y_hi: 2, y_lo: 4; y = y_hi * 4 + y_lo), z: 8, core: 2. Of those that a mesh axis runs over, the one named last changes fastest.
Arguments:
- scalar: float32 [64, 768, 768], P('gz', 'gy'), may hold values from -6 to 6
- velocity: float32 [3, 64, 256, 256], P(None, None, 'gy', 'gz'), may hold values from -0.9 to 0.9
Outputs:
- remeshed: float32 [64, 768, 768], P('gz', 'gy')
The draws below stay inside these ranges and needn't reach their ends.
All inputs are finite; a program needn't handle non-finite values.
Results may differ from the reference program's by a relative error of at most 0.0003.
Values sent between devices are 32-bit elements; how exact they have to be, the bound alone decides.
No kernel may reach another device: no remote copies, remote signals or barrier semaphores. Data moves between devices by JAX's collectives and lax.ppermute only.
A program may use at most 64 MiB of HBM per device.

```python
import jax
import jax.numpy as jnp
from jax import lax

NX = 768
NY = 768
NZ = 64
NXC = 256
NYC = 256


def level_of(stream_key, dims, cuts, smallest, high):
    factor_of = 1.0
    for position, shards_of in cuts:
        heights = jax.random.uniform(jax.random.fold_in(jax.random.fold_in(stream_key, 6), position), (shards_of,), jnp.float32, smallest / len(cuts), high / len(cuts))
        factor_of = factor_of * jnp.repeat(jnp.exp(heights), dims[position] // shards_of).reshape((-1,) + (1,) * (len(dims) - 1 - position))
    return factor_of


def bell_draw(stream_key, dims, scale, most, cuts=(), held_as=jnp.bfloat16):
    gain = level_of(stream_key, dims, cuts, -0.22, 0.18) if cuts else 1.0
    array = jax.random.normal(stream_key, dims, jnp.float32) * scale * gain
    return jnp.minimum(jnp.maximum(array, -most), most).astype(held_as)


def setup_inputs(seed: int = 0) -> dict:
    key_of = jax.random.split(jax.random.key(seed), 3)
    scalar = bell_draw(key_of[0], (NZ, NY, NX), 1.0, 6.0, ((0, 16), (1, 32)), jnp.float32)
    velocity = jnp.clip(jax.random.uniform(key_of[1], (3, NZ, NYC, NXC), jnp.float32, -0.9, 0.9) * level_of(key_of[1], (3, NZ, NYC, NXC), ((2, 32), (3, 16)), -0.4, 0.0), -0.9, 0.9)
    return {"scalar": scalar, "velocity": velocity}


def alternate(current, following, along):
    pieces = [current * (1.0 - phase / 3.0) + following * (phase / 3.0) for phase in range(3)]
    stacked = jnp.stack(pieces, axis=along + 1)
    new_shape = list(current.shape)
    new_shape[along] = new_shape[along] * 3
    return stacked.reshape(new_shape)


def polynomial(factors, value):
    result = jnp.zeros_like(value)
    for factor in reversed(factors):
        result = result * value + factor
    return result


def kernel_weight(offset):
    size = jnp.abs(offset)
    inner = polynomial([1.0, 0.0, -5.0 / 4.0, -35.0 / 12.0, 21.0 / 4.0, -25.0 / 12.0], size)
    middle = polynomial([-4.0, 75.0 / 4.0, -245.0 / 8.0, 545.0 / 24.0, -63.0 / 8.0, 25.0 / 24.0], size)
    outer = polynomial([18.0, -153.0 / 4.0, 255.0 / 8.0, -313.0 / 24.0, 21.0 / 8.0, -5.0 / 24.0], size)
    return jnp.where(size < 1.0, inner, jnp.where(size < 2.0, middle, jnp.where(size < 3.0, outer, 0.0)))


def displacement(speed, before, after):
    half_step = 0.5 * speed
    return jnp.where(half_step >= 0.0, (1.0 - half_step) * speed + half_step * after, (1.0 + half_step) * speed - half_step * before)


def sweep_periodic(field, speed, along):
    moved = displacement(speed, jnp.roll(speed, 1, along), jnp.roll(speed, -1, along))
    result = jnp.zeros_like(field)
    for offset in range(-3, 4):
        result = result + jnp.roll(field * kernel_weight(offset - moved), offset, along)
    return result


def sweep_open(field, speed):
    zero_plane = jnp.zeros_like(speed[:1])
    before = jnp.concatenate([zero_plane, speed[:-1]], axis=0)
    after = jnp.concatenate([speed[1:], zero_plane], axis=0)
    moved = displacement(speed, before, after)
    count = field.shape[0]
    total = jnp.zeros((count + 6,) + field.shape[1:], jnp.float32)
    for offset in range(-3, 4):
        total = total.at[3 + offset:3 + offset + count].add(field * kernel_weight(offset - moved))
    return total[3:3 + count]


def plane_sweeps(pair):
    plane, coarse = pair
    y_fine = alternate(coarse, jnp.roll(coarse, -1, 1), 1)
    fine_vel = alternate(y_fine, jnp.roll(y_fine, -1, 2), 2)
    field = sweep_periodic(plane, fine_vel[0], 1)
    field = sweep_periodic(field, fine_vel[1], 0)
    return field.T, fine_vel[2].T


def column_sweep(pair):
    return sweep_open(pair[0], pair[1])


def reference(scalar, velocity):
    swept, vertical = lax.map(plane_sweeps, (scalar, jnp.moveaxis(velocity, 1, 0)))
    columns = lax.map(column_sweep, (jnp.moveaxis(swept, 1, 0), jnp.moveaxis(vertical, 1, 0)))
    return jnp.moveaxis(columns, 0, 1)
```

```python
import jax
import jax.numpy as jnp
from jax import lax
from jax.experimental import pallas as pl
from jax.experimental.pallas import tpu as pltpu
from jax.sharding import PartitionSpec as P

F32 = jnp.float32
BF16 = jnp.bfloat16


def iota(shape, dim):
    return lax.broadcasted_iota(jnp.int32, shape, dim)


def remesh_terms(u, before, after, q):
    up = u >= 0.0
    size = jnp.abs(u)
    a = size - (0.5 * size) * (size - jnp.where(up, after, -before))
    b = a - 0.5
    s = b * b
    e1 = (-1.0 / 16.0 * s + 13.0 / 32.0) * s - 25.0 / 256.0
    e2 = (1.0 / 48.0 * s - 5.0 / 96.0) * s + 3.0 / 256.0
    e0 = 0.5 - e1 - e2
    o0 = ((-25.0 / 12.0 * s + 19.0 / 8.0) * s - 281.0 / 192.0) * b
    o1 = ((25.0 / 24.0 * s - 53.0 / 48.0) * s + 27.0 / 128.0) * b
    o2 = ((-5.0 / 24.0 * s + 3.0 / 16.0) * s - 13.0 / 384.0) * b
    at0 = q * (e0 + o0)
    near1, far1 = q * (e0 - o0), q * (e1 + o1)
    near2, far2 = q * (e1 - o1), q * (e2 + o2)
    near3 = q * (e2 - o2)
    zero = jnp.zeros_like(q)
    return {
        0: at0,
        1: jnp.where(up, near1, far1),
        -1: jnp.where(up, far1, near1),
        2: jnp.where(up, near2, far2),
        -2: jnp.where(up, far2, near2),
        3: jnp.where(up, near3, zero),
        -3: jnp.where(up, zero, near3),
    }


def roll(x, shift, axis):
    n = x.shape[axis]
    shift = shift % n
    return x if shift == 0 else pltpu.roll(x, shift, axis)


def sweep_ring(q, u, axis):
    terms = remesh_terms(u, roll(u, 1, axis), roll(u, -1, axis), q)
    total = terms[0]
    for m in (1, -1, 2, -2, 3, -3):
        total = total + roll(terms[m], m, axis)
    return total


def pack_velocity(v_ref, out_ref):
    blank = jnp.zeros((8, 16), F32)
    for k in range(16):
        planes = [v_ref[c, 4 * k + p] for c in range(2) for p in range(4)]
        out_ref[k, 0:8, :] = jnp.concatenate(planes, axis=1)
        planes = [v_ref[2, z] if 0 <= z < 64 else blank for z in range(4 * k - 1, 4 * k + 5)]
        out_ref[k, 8:16, :] = jnp.concatenate(planes + [blank, blank], axis=1)


def pack_scalar(s_ref, out_ref, t_ref):
    for v in range(6):
        block = s_ref[:, :, 128 * v : 128 * v + 128].reshape(96, 128)
        block = jnp.concatenate([block, jnp.zeros((32, 128), F32)], axis=0)
        t_ref[128 * v : 128 * v + 128, :] = block.T
    lane = iota((8, 128), 1)
    row = iota((8, 128), 0)
    for i in range(32):
        left = t_ref[(24 * i - 8) % 768 : (24 * i - 8) % 768 + 8, :]
        right = t_ref[(24 * i + 24) % 768 : (24 * i + 24) % 768 + 8, :]
        halo = jnp.where(row < 4, right, left)
        for t in range(3):
            tile = t_ref[24 * i + 8 * t : 24 * i + 8 * t + 8, :]
            out_ref[i, 8 * t : 8 * t + 8, :] = jnp.where(lane < 96, tile, roll(halo, 96 - 32 * t, 1))


def spread_velocity(r_ref, out_ref):
    col = iota((8, 128), 1) & 15
    for i in range(32):
        k = i // 2
        for g in range(2):
            here = r_ref[k, 8 * g : 8 * g + 8, :]
            if i % 2 == 0:
                other = r_ref[(k - 1) % 16, 8 * g : 8 * g + 8, :]
                tile = jnp.where(col == 0, roll(other, -15, 1), roll(here, 1, 1))
            else:
                other = r_ref[(k + 1) % 16, 8 * g : 8 * g + 8, :]
                tile = jnp.where(col < 9, roll(here, -7, 1), roll(other, 9, 1))
            out_ref[i, 8 * g : 8 * g + 8, :] = tile


def pieces(x):
    hi = x.astype(BF16)
    rest = x - hi.astype(F32)
    mid = rest.astype(BF16)
    return hi, mid, (rest - mid.astype(F32)).astype(BF16)


def split_dot(left, right, split_left):
    total = None
    for part in pieces(left if split_left else right)[::-1]:
        pair = (part, right) if split_left else (left, part)
        term = jnp.dot(*pair, preferred_element_type=F32)
        total = term if total is None else total + term
    return total


def hat_rows(rows, slot, ring):
    e = iota((rows, 128), 0)
    if ring:
        e = jnp.where(e > 28, e - 32, e)
    lane = iota((rows, 128), 1)
    away = jnp.abs(e - 3 * ((lane & 15) - 1))
    return jnp.where((lane >> 4) == slot, jnp.maximum(3 - away, 0), 0).astype(F32).astype(BF16)


def sweeps(s_ref, v_ref, own_ref, up_ref, down_ref, my_ref, f_ref, ux_ref, uy_ref, uz_ref, x_ref, y_ref):
    for v in range(6):
        c = iota((256, 128), 0)
        f = iota((256, 128), 1) + 128 * v
        away = jnp.abs(f - 3 * c)
        away = jnp.minimum(away, 768 - away)
        my_ref[:, 128 * v : 128 * v + 128] = jnp.maximum(3 - away, 0).astype(F32).astype(BF16)
    my = my_ref[...]
    xy = jnp.concatenate([hat_rows(32, p, True) for p in range(4)] + [hat_rows(24, 4 + p, False) for p in range(4)], axis=0)
    zz = jnp.concatenate([hat_rows(24, p, False) for p in range(6)], axis=0)
    for g in range(2):
        coarse = v_ref[:, 8 * g : 8 * g + 8, :].reshape(256, 128)
        fine_y = split_dot(coarse.T, my, True)
        fine = split_dot(xy if g == 0 else zz, fine_y, False) * (1.0 / 9.0)
        if g == 0:
            ux_ref[...] = fine[:128].reshape(4, 32, 768)
            uy_ref[...] = fine[128:].reshape(4, 24, 768)
        else:
            uz_ref[...] = fine.reshape(6, 24, 768)
    lane = iota((8, 128), 1)
    for i in range(32):
        tiles = [s_ref[i, 8 * t : 8 * t + 8, :] for t in range(3)]
        halo = jnp.where(lane < 32, roll(tiles[0], -96, 1), jnp.where(lane < 64, roll(tiles[1], -64, 1), roll(tiles[2], -32, 1)))
        for t, tile in enumerate(tiles + [halo]):
            for p in range(4):
                v, at = divmod(24 * i, 128)
                moved = roll(tile, at - 24 * p, 1)
                here = min(24, 128 - at)
                f_ref[p, 8 * t : 8 * t + 8, 128 * v + at : 128 * v + at + here] = moved[:, at : at + here]
                if here < 24:
                    f_ref[p, 8 * t : 8 * t + 8, 128 * v + 128 : 128 * v + 128 + 24 - here] = moved[:, : 24 - here]
    for p in range(4):
        for v in range(6):
            part = slice(128 * v, 128 * v + 128)
            x_ref[p, :, part] = sweep_ring(f_ref[p, :, part], ux_ref[p, :, part], 0)[:24]
    for p in range(4):
        for t in range(3):
            rows = slice(8 * t, 8 * t + 8)
            y_ref[p, rows, :] = sweep_ring(x_ref[p, rows, :], uy_ref[p, rows, :], 1)
    for t in range(3):
        rows = slice(8 * t, 8 * t + 8)
        for v in range(6):
            part = slice(128 * v, 128 * v + 128)
            speeds = [uz_ref[p, rows, part] for p in range(6)]
            total = {}
            for p in range(4):
                terms = remesh_terms(speeds[p + 1], speeds[p], speeds[p + 2], y_ref[p, rows, part])
                for m, term in terms.items():
                    total[p + m] = total[p + m] + term if p + m in total else term
            for j in range(3):
                down_ref[j, rows, part] = total[j - 3]
                up_ref[j, rows, part] = total[j + 4]
            for j in range(4):
                own_ref[j, rows, part] = total[j]


def join(own_ref, low_ref, high_ref, out_ref):
    out_ref[0] = own_ref[0] + low_ref[0]
    out_ref[1] = own_ref[1] + low_ref[1] + high_ref[0]
    out_ref[2] = own_ref[2] + low_ref[2] + high_ref[1]
    out_ref[3] = own_ref[3] + high_ref[2]


def kernel(body, *shapes, scratch=()):
    outs = tuple(jax.ShapeDtypeStruct(s, F32) for s in shapes)
    return pl.pallas_call(
        body,
        out_shape=outs if len(outs) > 1 else outs[0],
        scratch_shapes=[pltpu.VMEM(s, d) for s, d in scratch],
    )


def exchange(x, axis):
    return lax.all_to_all(x, axis, split_axis=0, concat_axis=0, tiled=False)


def local(scalar, velocity):
    chunks = kernel(pack_velocity, (16, 16, 128))(velocity)
    planes = exchange(chunks, "gz")
    field = exchange(kernel(pack_scalar, (32, 24, 128), scratch=[((768, 128), F32)])(scalar), "gy")
    speeds = exchange(kernel(spread_velocity, (32, 16, 128))(planes), "gy")
    own, up, down = kernel(
        sweeps,
        (4, 24, 768),
        (3, 24, 768),
        (3, 24, 768),
        scratch=[
            ((256, 768), BF16),
            ((4, 32, 768), F32),
            ((4, 32, 768), F32),
            ((4, 24, 768), F32),
            ((6, 24, 768), F32),
            ((4, 24, 768), F32),
            ((4, 24, 768), F32),
        ],
    )(field, speeds)
    steps = [(k, k + 1) for k in range(lax.axis_size("gz") - 1)]
    low = lax.ppermute(up, "gz", steps)
    high = lax.ppermute(down, "gz", [(b, a) for a, b in steps])
    return kernel(join, (4, 24, 768))(own, low, high)


def solution(mesh):
    in_specs = (P("gz", "gy", None), P(None, None, "gy", "gz"))
    out_specs = P("gz", "gy", None)
    return jax.shard_map(local, mesh=mesh, in_specs=in_specs, out_specs=out_specs, check_vma=False)
```

```python
import jax
import jax.numpy as jnp
from jax import lax
from jax.experimental import pallas as pl
from jax.experimental.pallas import tpu as pltpu
from jax.sharding import PartitionSpec as P

F32 = jnp.float32
BF16 = jnp.bfloat16


def iota(shape, dim):
    return lax.broadcasted_iota(jnp.int32, shape, dim)


def remesh_terms(u, before, after, q):
    up = u >= 0.0
    size = jnp.abs(u)
    a = size - (0.5 * size) * (size - jnp.where(up, after, -before))
    b = a - 0.5
    s = b * b
    e1 = (-1.0 / 16.0 * s + 13.0 / 32.0) * s - 25.0 / 256.0
    e2 = (1.0 / 48.0 * s - 5.0 / 96.0) * s + 3.0 / 256.0
    e0 = 0.5 - e1 - e2
    o0 = ((-25.0 / 12.0 * s + 19.0 / 8.0) * s - 281.0 / 192.0) * b
    o1 = ((25.0 / 24.0 * s - 53.0 / 48.0) * s + 27.0 / 128.0) * b
    o2 = ((-5.0 / 24.0 * s + 3.0 / 16.0) * s - 13.0 / 384.0) * b
    at0 = q * (e0 + o0)
    near1, far1 = q * (e0 - o0), q * (e1 + o1)
    near2, far2 = q * (e1 - o1), q * (e2 + o2)
    near3 = q * (e2 - o2)
    zero = jnp.zeros_like(q)
    return {
        0: at0,
        1: jnp.where(up, near1, far1),
        -1: jnp.where(up, far1, near1),
        2: jnp.where(up, near2, far2),
        -2: jnp.where(up, far2, near2),
        3: jnp.where(up, near3, zero),
        -3: jnp.where(up, zero, near3),
    }


def roll(x, shift, axis):
    n = x.shape[axis]
    shift = shift % n
    return x if shift == 0 else pltpu.roll(x, shift, axis)


def sweep_ring(q, u, axis):
    terms = remesh_terms(u, roll(u, 1, axis), roll(u, -1, axis), q)
    total = terms[0]
    for m in (1, -1, 2, -2, 3, -3):
        total = total + roll(terms[m], m, axis)
    return total


def swap_blocks(x):
    row = iota((8, 128), 0)
    block = iota((8, 128), 1) >> 4
    for bit in (1, 2, 4):
        low = (row & bit) == 0
        first = (block & bit) == 0
        upward = roll(roll(x, -bit, 0), 16 * bit, 1)
        downward = roll(roll(x, bit, 0), -16 * bit, 1)
        x = jnp.where(low == first, x, jnp.where(low, upward, downward))
    return x


def pack_velocity(v_ref, out_ref):
    lane = iota((8, 128), 1)
    tiles = []
    for c in range(3):
        block = v_ref[c].reshape(128, 64)
        block = jnp.concatenate([block, jnp.zeros((128, 64), F32)], axis=1).T
        tiles.append([swap_blocks(block[8 * n : 8 * n + 8]) for n in range(8)])
    zero = jnp.zeros((8, 128), F32)
    for k in range(16):
        n, odd = divmod(k, 2)
        if odd == 0:
            out_ref[k, 0:8, :] = jnp.where(lane < 64, tiles[0][n], roll(tiles[1][n], 64, 1))
            before = tiles[2][n - 1] if n > 0 else zero
            planes = jnp.where(lane < 16, roll(before, 16, 1), roll(tiles[2][n], 16, 1))
        else:
            out_ref[k, 0:8, :] = jnp.where(lane < 64, roll(tiles[0][n], -64, 1), tiles[1][n])
            after = tiles[2][n + 1] if n < 7 else zero
            planes = jnp.where(lane < 80, roll(tiles[2][n], -48, 1), roll(after, 80, 1))
        out_ref[k, 8:16, :] = jnp.where(lane < 96, planes, zero)


def pack_chunks(s_ref, r_ref, out_ref, t_ref):
    for v in range(6):
        block = s_ref[:, :, 128 * v : 128 * v + 128].reshape(96, 128)
        block = jnp.concatenate([block, jnp.zeros((32, 128), F32)], axis=0)
        t_ref[128 * v : 128 * v + 128, :] = block.T
    lane = iota((8, 128), 1)
    row = iota((8, 128), 0)
    col = lane & 15
    slot = lane >> 4
    for i in range(32):
        k = i // 2
        here, depth = r_ref[k, 0:8, :], r_ref[k, 8:16, :]
        if i % 2 == 0:
            other = r_ref[(k - 1) % 16, 0:8, :]
            wide = jnp.where(col == 0, roll(other, -15, 1), roll(here, 1, 1))
            near = here
        else:
            other = r_ref[(k + 1) % 16, 0:8, :]
            wide = jnp.where(col < 9, roll(here, -7, 1), roll(other, 9, 1))
            near = jnp.where(col < 8, roll(here, -8, 1), roll(other, 8, 1))
            depth = jnp.where(col < 8, roll(depth, -8, 1), roll(r_ref[(k + 1) % 16, 8:16, :], 8, 1))
        tile = jnp.where(slot < 4, wide, near)
        tile = jnp.where((slot >= 4) & (col >= 9), roll(depth, 73, 1), tile)
        tile = jnp.where((slot < 2) & (col >= 11), roll(depth, -53, 1), tile)
        tile = jnp.where(((slot >> 1) == 1) & (col >= 11), roll(depth, -26, 1), tile)
        out_ref[i, 24:32, :] = tile
        rest = jnp.where((slot < 4) & ((col == 7) | (col == 8)), depth, 0.0)
        rest = pltpu.roll(rest, 0, 1, stride=2, stride_axis=0)
        stash = jnp.sum(rest, axis=0, keepdims=True)
        left = t_ref[(24 * i - 8) % 768 : (24 * i - 8) % 768 + 8, :]
        right = t_ref[(24 * i + 24) % 768 : (24 * i + 24) % 768 + 8, :]
        halo = jnp.where(row < 3, right, jnp.where(row == 3, stash, left))
        for t in range(3):
            tile = t_ref[24 * i + 8 * t : 24 * i + 8 * t + 8, :]
            out_ref[i, 8 * t : 8 * t + 8, :] = jnp.where(lane < 96, tile, roll(halo, 96 - 32 * t, 1))


def pieces(x):
    hi = x.astype(BF16)
    rest = x - hi.astype(F32)
    mid = rest.astype(BF16)
    return hi, mid, (rest - mid.astype(F32)).astype(BF16)


def split_dot(left, right, split_left):
    total = None
    for part in pieces(left if split_left else right)[::-1]:
        pair = (part, right) if split_left else (left, part)
        term = jnp.dot(*pair, preferred_element_type=F32)
        total = term if total is None else total + term
    return total


def hat_rows(rows, slot, ring):
    e = iota((rows, 128), 0)
    if ring:
        e = jnp.where(e > 28, e - 32, e) + 3
    lane = iota((rows, 128), 1)
    away = jnp.abs(e - 3 * (lane & 15))
    return jnp.where((lane >> 4) == slot, jnp.maximum(3 - away, 0), 0).astype(F32).astype(BF16)


def sweeps(s_ref, own_ref, up_ref, down_ref, my_ref, c_ref, f_ref, ux_ref, uy_ref, uz_ref, x_ref, y_ref):
    lane = iota((8, 128), 1)
    row = iota((8, 128), 0)
    col = lane & 15
    slot = lane >> 4
    for i in range(32):
        tiles = [s_ref[i, 8 * t : 8 * t + 8, :] for t in range(3)]
        halo = jnp.where(lane < 32, roll(tiles[0], -96, 1), jnp.where(lane < 64, roll(tiles[1], -64, 1), roll(tiles[2], -32, 1)))
        for t, tile in enumerate(tiles + [halo]):
            for p in range(4):
                v, at = divmod(24 * i, 128)
                moved = roll(tile, at - 24 * p, 1)
                here = min(24, 128 - at)
                f_ref[p, 8 * t : 8 * t + 8, 128 * v + at : 128 * v + at + here] = moved[:, at : at + here]
                if here < 24:
                    f_ref[p, 8 * t : 8 * t + 8, 128 * v + 128 : 128 * v + 128 + 24 - here] = moved[:, : 24 - here]
        packed = s_ref[i, 24:32, :]
        rest = jnp.broadcast_to(halo[3:4, :], (8, 128))
        for bit in (1, 2, 4):
            rest = jnp.where((row & bit) == 0, rest, roll(rest, -2 * bit, 1))
        depth = jnp.where(slot >= 4, jnp.where(col < 5, roll(packed, 53, 1), roll(packed, 26, 1)), jnp.where(col < 7, roll(packed, -73, 1), rest))
        c_ref[0, 8 * i : 8 * i + 8, :] = packed
        c_ref[1, 8 * i : 8 * i + 8, :] = depth
    for v in range(6):
        c = iota((256, 128), 0)
        f = iota((256, 128), 1) + 128 * v
        away = jnp.abs(f - 3 * c)
        away = jnp.minimum(away, 768 - away)
        my_ref[:, 128 * v : 128 * v + 128] = jnp.maximum(3 - away, 0).astype(F32).astype(BF16)
    my = my_ref[...]
    xy = jnp.concatenate([hat_rows(32, p, True) for p in range(4)] + [hat_rows(24, 4 + p, False) for p in range(4)], axis=0)
    zz = jnp.concatenate([hat_rows(24, p, False) for p in range(6)], axis=0)
    for g in range(2):
        fine_y = split_dot(c_ref[g].T, my, True)
        fine = split_dot(xy if g == 0 else zz, fine_y, False) * (1.0 / 9.0)
        if g == 0:
            ux_ref[...] = fine[:128].reshape(4, 32, 768)
            uy_ref[...] = fine[128:].reshape(4, 24, 768)
        else:
            uz_ref[...] = fine.reshape(6, 24, 768)
    for p in range(4):
        for v in range(6):
            part = slice(128 * v, 128 * v + 128)
            x_ref[p, :, part] = sweep_ring(f_ref[p, :, part], ux_ref[p, :, part], 0)[:24]
    for p in range(4):
        for t in range(3):
            rows = slice(8 * t, 8 * t + 8)
            y_ref[p, rows, :] = sweep_ring(x_ref[p, rows, :], uy_ref[p, rows, :], 1)
    for t in range(3):
        rows = slice(8 * t, 8 * t + 8)
        for v in range(6):
            part = slice(128 * v, 128 * v + 128)
            speeds = [uz_ref[p, rows, part] for p in range(6)]
            total = {}
            for p in range(4):
                terms = remesh_terms(speeds[p + 1], speeds[p], speeds[p + 2], y_ref[p, rows, part])
                for m, term in terms.items():
                    total[p + m] = total[p + m] + term if p + m in total else term
            for j in range(3):
                down_ref[j, rows, part] = total[j - 3]
                up_ref[j, rows, part] = total[j + 4]
            for j in range(4):
                own_ref[j, rows, part] = total[j]


def join(own_ref, low_ref, high_ref, out_ref):
    out_ref[0] = own_ref[0] + low_ref[0]
    out_ref[1] = own_ref[1] + low_ref[1] + high_ref[0]
    out_ref[2] = own_ref[2] + low_ref[2] + high_ref[1]
    out_ref[3] = own_ref[3] + high_ref[2]


def kernel(body, *shapes, scratch=()):
    outs = tuple(jax.ShapeDtypeStruct(s, F32) for s in shapes)
    return pl.pallas_call(
        body,
        out_shape=outs if len(outs) > 1 else outs[0],
        scratch_shapes=[pltpu.VMEM(s, d) for s, d in scratch],
        compiler_params=pltpu.CompilerParams(vmem_limit_bytes=16 * 1024 * 1024),
    )


def exchange(x, axis):
    return lax.all_to_all(x, axis, split_axis=0, concat_axis=0, tiled=False)


def local(scalar, velocity):
    planes = exchange(kernel(pack_velocity, (16, 16, 128))(jnp.transpose(velocity, (0, 2, 3, 1))), "gz")
    chunks = exchange(kernel(pack_chunks, (32, 32, 128), scratch=[((768, 128), F32)])(scalar, planes), "gy")
    own, up, down = kernel(
        sweeps,
        (4, 24, 768),
        (3, 24, 768),
        (3, 24, 768),
        scratch=[
            ((256, 768), BF16),
            ((2, 256, 128), F32),
            ((4, 32, 768), F32),
            ((4, 32, 768), F32),
            ((4, 24, 768), F32),
            ((6, 24, 768), F32),
            ((4, 24, 768), F32),
            ((4, 24, 768), F32),
        ],
    )(chunks)
    steps = [(k, k + 1) for k in range(lax.axis_size("gz") - 1)]
    low = lax.ppermute(up, "gz", steps)
    high = lax.ppermute(down, "gz", [(b, a) for a, b in steps])
    return kernel(join, (4, 24, 768))(own, low, high)


def solution(mesh):
    in_specs = (P("gz", "gy", None), P(None, None, "gy", "gz"))
    out_specs = P("gz", "gy", None)
    return jax.shard_map(local, mesh=mesh, in_specs=in_specs, out_specs=out_specs, check_vma=False)
```

```python
import jax
import jax.numpy as jnp
from jax import lax
from jax.experimental import pallas as pl
from jax.experimental.pallas import tpu as pltpu
from jax.sharding import PartitionSpec as P


F32 = jnp.float32
BF16 = jnp.bfloat16


def iota(shape, dim):
    return lax.broadcasted_iota(jnp.int32, shape, dim)


def remesh_terms(u, before, after, q):
    up = u >= 0.0
    size = jnp.abs(u)
    a = size - (0.5 * size) * (size - jnp.where(up, after, -before))
    b = a - 0.5
    s = b * b
    e1 = (-1.0 / 16.0 * s + 13.0 / 32.0) * s - 25.0 / 256.0
    e2 = (1.0 / 48.0 * s - 5.0 / 96.0) * s + 3.0 / 256.0
    e0 = 0.5 - e1 - e2
    o0 = ((-25.0 / 12.0 * s + 19.0 / 8.0) * s - 281.0 / 192.0) * b
    o1 = ((25.0 / 24.0 * s - 53.0 / 48.0) * s + 27.0 / 128.0) * b
    o2 = ((-5.0 / 24.0 * s + 3.0 / 16.0) * s - 13.0 / 384.0) * b
    at0 = q * (e0 + o0)
    near1, far1 = q * (e0 - o0), q * (e1 + o1)
    near2, far2 = q * (e1 - o1), q * (e2 + o2)
    near3 = q * (e2 - o2)
    zero = jnp.zeros_like(q)
    return {
        0: at0,
        1: jnp.where(up, near1, far1),
        -1: jnp.where(up, far1, near1),
        2: jnp.where(up, near2, far2),
        -2: jnp.where(up, far2, near2),
        3: jnp.where(up, near3, zero),
        -3: jnp.where(up, zero, near3),
    }


def roll(x, shift, axis):
    n = x.shape[axis]
    shift = shift % n
    return x if shift == 0 else pltpu.roll(x, shift, axis)


def sweep_ring(q, u, axis):
    terms = remesh_terms(u, roll(u, 1, axis), roll(u, -1, axis), q)
    total = terms[0]
    for m in (1, -1, 2, -2, 3, -3):
        total = total + roll(terms[m], m, axis)
    return total


def swap_blocks(x):
    row = iota((8, 128), 0)
    block = iota((8, 128), 1) >> 4
    for bit in (1, 2, 4):
        low = (row & bit) == 0
        first = (block & bit) == 0
        upward = roll(roll(x, -bit, 0), 16 * bit, 1)
        downward = roll(roll(x, bit, 0), -16 * bit, 1)
        x = jnp.where(low == first, x, jnp.where(low, upward, downward))
    return x


def pack_velocity(v_ref, out_ref):
    lane = iota((8, 128), 1)
    tiles = []
    for c in range(3):
        block = v_ref[c].reshape(128, 64)
        block = jnp.concatenate([block, jnp.zeros((128, 64), F32)], axis=1).T
        tiles.append([swap_blocks(block[8 * n : 8 * n + 8]) for n in range(8)])
    zero = jnp.zeros((8, 128), F32)
    for k in range(16):
        n, odd = divmod(k, 2)
        if odd == 0:
            out_ref[k, 0:8, :] = jnp.where(lane < 64, tiles[0][n], roll(tiles[1][n], 64, 1))
            before = tiles[2][n - 1] if n > 0 else zero
            planes = jnp.where(lane < 16, roll(before, 16, 1), roll(tiles[2][n], 16, 1))
        else:
            out_ref[k, 0:8, :] = jnp.where(lane < 64, roll(tiles[0][n], -64, 1), tiles[1][n])
            after = tiles[2][n + 1] if n < 7 else zero
            planes = jnp.where(lane < 80, roll(tiles[2][n], -48, 1), roll(after, 80, 1))
        out_ref[k, 8:16, :] = jnp.where(lane < 96, planes, zero)


def odd_device():
    return lax.axis_index("gz") & 1


def pack_scalar(s_ref, out_ref, t_ref):
    flip = odd_device() * 3
    for v in range(6):
        part = slice(128 * v, 128 * v + 128)
        block = jnp.concatenate([s_ref[p ^ flip, :, part] for p in range(4)] + [jnp.zeros((32, 128), F32)], axis=0)
        t_ref[part, :] = block.T
    lane = iota((8, 128), 1)
    row = iota((8, 128), 0)
    for i in range(32):
        left = t_ref[(24 * i - 8) % 768 : (24 * i - 8) % 768 + 8, :]
        right = t_ref[(24 * i + 24) % 768 : (24 * i + 24) % 768 + 8, :]
        halo = jnp.where(row < 4, right, left)
        for t in range(3):
            tile = t_ref[24 * i + 8 * t : 24 * i + 8 * t + 8, :]
            out_ref[i, 8 * t : 8 * t + 8, :] = jnp.where(lane < 96, tile, roll(halo, 96 - 32 * t, 1))


def add_velocity(old_ref, r_ref, out_ref):
    lane = iota((8, 128), 1)
    row = iota((8, 128), 0)
    col = lane & 15
    slot = lane >> 4
    for i in range(32):
        k = i // 2
        here, depth = r_ref[k, 0:8, :], r_ref[k, 8:16, :]
        if i % 2 == 0:
            other = r_ref[(k - 1) % 16, 0:8, :]
            wide = jnp.where(col == 0, roll(other, -15, 1), roll(here, 1, 1))
            near = here
        else:
            other = r_ref[(k + 1) % 16, 0:8, :]
            wide = jnp.where(col < 9, roll(here, -7, 1), roll(other, 9, 1))
            near = jnp.where(col < 8, roll(here, -8, 1), roll(other, 8, 1))
            depth = jnp.where(col < 8, roll(depth, -8, 1), roll(r_ref[(k + 1) % 16, 8:16, :], 8, 1))
        tile = jnp.where(slot < 4, wide, near)
        tile = jnp.where((slot >= 4) & (col >= 9), roll(depth, 73, 1), tile)
        tile = jnp.where((slot < 2) & (col >= 11), roll(depth, -53, 1), tile)
        tile = jnp.where(((slot >> 1) == 1) & (col >= 11), roll(depth, -26, 1), tile)
        out_ref[i, 24:32, :] = tile
        rest = jnp.where((slot < 4) & ((col == 7) | (col == 8)), depth, 0.0)
        rest = pltpu.roll(rest, 0, 1, stride=2, stride_axis=0)
        stash = jnp.broadcast_to(jnp.sum(rest, axis=0, keepdims=True), (8, 128))
        for t in range(3):
            rows = slice(8 * t, 8 * t + 8)
            out_ref[i, rows, :] = jnp.where((row == 3) & (lane >= 96), roll(stash, 96 - 32 * t, 1), old_ref[i, rows, :])


def hat_rows(rows, slot, ring):
    e = iota((rows, 128), 0)
    if ring:
        e = jnp.where(e > 28, e - 32, e) + 3
    lane = iota((rows, 128), 1)
    away = jnp.abs(e - 3 * (lane & 15))
    return jnp.where((lane >> 4) == slot, jnp.maximum(3 - away, 0), 0)


def weights(y_ref, near_ref, near_z_ref, far_ref, far_z_ref):
    odd = odd_device()
    for v in range(6):
        c = iota((256, 128), 0)
        f = iota((256, 128), 1) + 128 * v
        away = jnp.abs(f - 3 * c)
        away = jnp.minimum(away, 768 - away)
        y_ref[:, 128 * v : 128 * v + 128] = jnp.maximum(3 - away, 0).astype(F32).astype(BF16)

    def both(rows):
        return jnp.concatenate(rows, axis=0).astype(F32).astype(BF16)

    sign = 1 - 2 * odd
    for planes, speeds, xy_ref, z_ref in (((0, 1, 2), range(5), near_ref, near_z_ref), ((3,), (3, 4, 5), far_ref, far_z_ref)):
        xy = both([hat_rows(32, p ^ (3 * odd), True) for p in planes] + [hat_rows(24, 4 + (p ^ (3 * odd)), False) for p in planes])
        z = both([hat_rows(24, jnp.where(odd == 1, 5 - p, p), False) * sign for p in speeds])
        xy_ref[:, 0:128] = xy
        xy_ref[:, 128:256] = xy
        z_ref[:, 0:128] = z
        z_ref[:, 128:256] = z


def two_pieces(x):
    hi = x.astype(BF16)
    return jnp.concatenate([hi, (x - hi.astype(F32)).astype(BF16)], axis=0)


def unpack(s_ref, f_ref, c_ref, planes):
    lane = iota((8, 128), 1)
    row = iota((8, 128), 0)
    col = lane & 15
    slot = lane >> 4
    for i in range(32):
        tiles = [s_ref[i, 8 * t : 8 * t + 8, :] for t in range(3)]
        halo = jnp.where(lane < 32, roll(tiles[0], -96, 1), jnp.where(lane < 64, roll(tiles[1], -64, 1), roll(tiles[2], -32, 1)))
        v, at = divmod(24 * i, 128)
        here = min(24, 128 - at)
        for t, tile in enumerate(tiles + [halo]):
            rows = slice(8 * t, 8 * t + 8)
            for n, p in enumerate(planes):
                moved = roll(tile, at - 24 * p, 1)
                f_ref[n, rows, 128 * v + at : 128 * v + at + here] = moved[:, at : at + here]
                if here < 24:
                    f_ref[n, rows, 128 * v + 128 : 128 * v + 128 + 24 - here] = moved[:, : 24 - here]
        packed = s_ref[i, 24:32, :]
        rest = jnp.broadcast_to(halo[3:4, :], (8, 128))
        for bit in (1, 2, 4):
            rest = jnp.where((row & bit) == 0, rest, roll(rest, -2 * bit, 1))
        depth = jnp.where(slot >= 4, jnp.where(col < 5, roll(packed, 53, 1), roll(packed, 26, 1)), jnp.where(col < 7, roll(packed, -73, 1), rest))
        c_ref[0, 8 * i : 8 * i + 8, :] = packed * (1.0 / 9.0)
        c_ref[1, 8 * i : 8 * i + 8, :] = depth * (1.0 / 9.0)


def refine(coarse, y_ref, hats_ref):
    both = jnp.dot(two_pieces(coarse.T), y_ref[...], preferred_element_type=F32)
    return jnp.dot(hats_ref[...], two_pieces(both[:128] + both[128:]), preferred_element_type=F32)


def plane_sweeps(f_ref, u_ref, x_ref, q_ref, count):
    def along_x(v, carry):
        part = pl.ds(pl.multiple_of(128 * v, 128), 128)
        for p in range(count):
            x_ref[p, :, part] = sweep_ring(f_ref[p, :, part], u_ref[32 * p : 32 * p + 32, part], 0)[:24]
        return carry

    lax.fori_loop(0, 6, along_x, 0)

    def along_y(t, carry):
        for p in range(count):
            rows = pl.ds(pl.multiple_of(8 * t, 8), 8)
            speed = u_ref[pl.ds(pl.multiple_of(32 * count + 24 * p + 8 * t, 8), 8), :]
            q_ref[p, rows, :] = sweep_ring(x_ref[p, rows, :], speed, 1)
        return carry

    lax.fori_loop(0, 3, along_y, 0)


def near_planes(s_ref, y_ref, hats_ref, hats_z_ref, outer_ref, own_ref, inner_ref, f_ref, c_ref, u_ref, w_ref, x_ref, q_ref):
    unpack(s_ref, f_ref, c_ref, (0, 1, 2))
    u_ref[...] = refine(c_ref[0], y_ref, hats_ref)
    w_ref[...] = refine(c_ref[1], y_ref, hats_z_ref)
    plane_sweeps(f_ref, u_ref, x_ref, q_ref, 3)

    def along_z(v, carry):
        part = pl.ds(pl.multiple_of(128 * v, 128), 128)
        for t in range(3):
            rows = slice(8 * t, 8 * t + 8)
            speeds = [w_ref[24 * p + 8 * t : 24 * p + 8 * t + 8, part] for p in range(5)]
            total = {}
            for p in range(3):
                terms = remesh_terms(speeds[p + 1], speeds[p], speeds[p + 2], q_ref[p, rows, part])
                for m, term in terms.items():
                    total[p + m] = total[p + m] + term if p + m in total else term
            for n in range(3):
                outer_ref[n, rows, part] = total[-1 - n]
            for n in range(4):
                own_ref[n, rows, part] = total[n]
            for n in range(2):
                inner_ref[n, rows, part] = total[4 + n]
        return carry

    lax.fori_loop(0, 6, along_z, 0)


def far_plane(s_ref, y_ref, hats_ref, hats_z_ref, some_ref, rest_ref, own_ref, inner_ref, f_ref, c_ref, u_ref, w_ref, x_ref, q_ref):
    unpack(s_ref, f_ref, c_ref, (3,))
    u_ref[...] = refine(c_ref[0], y_ref, hats_ref)
    w_ref[...] = refine(c_ref[1], y_ref, hats_z_ref)
    plane_sweeps(f_ref, u_ref, x_ref, q_ref, 1)

    def along_z(v, carry):
        part = pl.ds(pl.multiple_of(128 * v, 128), 128)
        for t in range(3):
            rows = slice(8 * t, 8 * t + 8)
            before, speed, after = [w_ref[24 * p + 8 * t : 24 * p + 8 * t + 8, part] for p in range(3)]
            terms = remesh_terms(speed, before, after, q_ref[0, rows, part])
            for n in range(4):
                own_ref[n, rows, part] = some_ref[n, rows, part] + terms[n - 3]
            for n in range(2):
                inner_ref[n, rows, part] = rest_ref[n, rows, part] + terms[1 + n]
            inner_ref[2, rows, part] = terms[3]
        return carry

    lax.fori_loop(0, 6, along_z, 0)


def join(own_ref, outer_ref, inner_ref, out_ref):
    flip = odd_device() * 3
    out_ref[0 ^ flip] = own_ref[0] + outer_ref[0]
    out_ref[1 ^ flip] = own_ref[1] + outer_ref[1] + inner_ref[2]
    out_ref[2 ^ flip] = own_ref[2] + outer_ref[2] + inner_ref[1]
    out_ref[3 ^ flip] = own_ref[3] + inner_ref[0]


def kernel(body, *shapes, scratch=(), alias=None, flops=1e7):
    outs = tuple(jax.ShapeDtypeStruct(*(s if isinstance(s[0], tuple) else (s, F32))) for s in shapes)
    return pl.pallas_call(
        body,
        out_shape=outs if len(outs) > 1 else outs[0],
        scratch_shapes=[pltpu.VMEM(s, F32) for s in scratch],
        input_output_aliases=alias or {},
        cost_estimate=pl.CostEstimate(flops=int(flops), transcendentals=0, bytes_accessed=1 << 20),
        compiler_params=pltpu.CompilerParams(vmem_limit_bytes=16 * 1024 * 1024),
    )


def exchange(x, axis):
    return lax.all_to_all(x, axis, split_axis=0, concat_axis=0, tiled=False)


def sweep_scratch(count, speeds):
    return [(count, 32, 768), (2, 256, 128), (56 * count, 768), (24 * speeds, 768), (count, 24, 768), (count, 24, 768)]


def steps(scalar, velocity):
    planes = exchange(kernel(pack_velocity, (16, 16, 128))(jnp.transpose(velocity, (0, 2, 3, 1))), "gz")
    chunks = kernel(pack_scalar, (32, 32, 128), scratch=[(768, 128)])(scalar)
    tables = ((256, 768), (168, 256), (120, 256), (56, 256), (72, 256))
    y_weights, near, near_z, far, far_z = kernel(weights, *((s, BF16) for s in tables))()
    chunks = exchange(kernel(add_velocity, (32, 32, 128), alias={0: 0})(chunks, planes), "gy")
    outer, own, inner = kernel(near_planes, (3, 24, 768), (4, 24, 768), (2, 24, 768), scratch=sweep_scratch(3, 5))(chunks, y_weights, near, near_z)
    count = lax.axis_size("gz")
    pairs = [(k, k + 1) for k in range(1, count - 1, 2)]
    outer = lax.ppermute(outer, "gz", pairs + [(b, a) for a, b in pairs])
    own, inner = kernel(far_plane, (4, 24, 768), (3, 24, 768), scratch=sweep_scratch(1, 3), flops=1e9)(chunks, y_weights, far, far_z, own, inner)
    pairs = [(k, k + 1) for k in range(0, count, 2)]
    inner = lax.ppermute(inner, "gz", pairs + [(b, a) for a, b in pairs])
    return kernel(join, (4, 24, 768))(own, outer, inner)


def solution(mesh):
    in_specs = (P("gz", "gy", None), P(None, None, "gy", "gz"))
    out_specs = P("gz", "gy", None)
    return jax.shard_map(steps, mesh=mesh, in_specs=in_specs, out_specs=out_specs, check_vma=False)
```

```python
import jax
import jax.numpy as jnp
from jax import lax
from jax.experimental import pallas as pl
from jax.experimental.pallas import tpu as pltpu
from jax.sharding import PartitionSpec as P


F32 = jnp.float32
BF16 = jnp.bfloat16


def iota(shape, dim):
    return lax.broadcasted_iota(jnp.int32, shape, dim)


def remesh_terms(u, before, after, q):
    up = u >= 0.0
    size = jnp.abs(u)
    a = size - (0.5 * size) * (size - jnp.where(up, after, -before))
    b = a - 0.5
    s = b * b
    e1 = (-1.0 / 16.0 * s + 13.0 / 32.0) * s - 25.0 / 256.0
    e2 = (1.0 / 48.0 * s - 5.0 / 96.0) * s + 3.0 / 256.0
    e0 = 0.5 - e1 - e2
    o0 = ((-25.0 / 12.0 * s + 19.0 / 8.0) * s - 281.0 / 192.0) * b
    o1 = ((25.0 / 24.0 * s - 53.0 / 48.0) * s + 27.0 / 128.0) * b
    o2 = ((-5.0 / 24.0 * s + 3.0 / 16.0) * s - 13.0 / 384.0) * b
    at0 = q * (e0 + o0)
    near1, far1 = q * (e0 - o0), q * (e1 + o1)
    near2, far2 = q * (e1 - o1), q * (e2 + o2)
    near3 = q * (e2 - o2)
    zero = jnp.zeros_like(q)
    return {
        0: at0,
        1: jnp.where(up, near1, far1),
        -1: jnp.where(up, far1, near1),
        2: jnp.where(up, near2, far2),
        -2: jnp.where(up, far2, near2),
        3: jnp.where(up, near3, zero),
        -3: jnp.where(up, zero, near3),
    }


def roll(x, shift, axis):
    n = x.shape[axis]
    shift = shift % n
    return x if shift == 0 else pltpu.roll(x, shift, axis)


def sweep_ring(q, u, axis):
    terms = remesh_terms(u, roll(u, 1, axis), roll(u, -1, axis), q)
    total = terms[0]
    for m in (1, -1, 2, -2, 3, -3):
        total = total + roll(terms[m], m, axis)
    return total


def swap_blocks(x):
    row = iota((8, 128), 0)
    block = iota((8, 128), 1) >> 4
    for bit in (1, 2, 4):
        low = (row & bit) == 0
        first = (block & bit) == 0
        upward = roll(roll(x, -bit, 0), 16 * bit, 1)
        downward = roll(roll(x, bit, 0), -16 * bit, 1)
        x = jnp.where(low == first, x, jnp.where(low, upward, downward))
    return x


def pack_velocity(v_ref, out_ref):
    lane = iota((8, 128), 1)
    tiles = []
    for c in range(3):
        block = v_ref[c].reshape(128, 64)
        block = jnp.concatenate([block, jnp.zeros((128, 64), F32)], axis=1).T
        tiles.append([swap_blocks(block[8 * n : 8 * n + 8]) for n in range(8)])
    zero = jnp.zeros((8, 128), F32)
    for k in range(16):
        n, odd = divmod(k, 2)
        if odd == 0:
            out_ref[k, 0:8, :] = jnp.where(lane < 64, tiles[0][n], roll(tiles[1][n], 64, 1))
            before = tiles[2][n - 1] if n > 0 else zero
            planes = jnp.where(lane < 16, roll(before, 16, 1), roll(tiles[2][n], 16, 1))
        else:
            out_ref[k, 0:8, :] = jnp.where(lane < 64, roll(tiles[0][n], -64, 1), tiles[1][n])
            after = tiles[2][n + 1] if n < 7 else zero
            planes = jnp.where(lane < 80, roll(tiles[2][n], -48, 1), roll(after, 80, 1))
        out_ref[k, 8:16, :] = jnp.where(lane < 96, planes, zero)


def odd_device():
    return lax.axis_index("gz") & 1


def pack_scalar(s_ref, out_ref, t_ref):
    flip = odd_device() * 3
    for v in range(6):
        part = slice(128 * v, 128 * v + 128)
        block = jnp.concatenate([s_ref[p ^ flip, :, part] for p in range(4)] + [jnp.zeros((32, 128), F32)], axis=0)
        t_ref[part, :] = block.T
    lane = iota((8, 128), 1)
    row = iota((8, 128), 0)
    for i in range(32):
        left = t_ref[(24 * i - 8) % 768 : (24 * i - 8) % 768 + 8, :]
        right = t_ref[(24 * i + 24) % 768 : (24 * i + 24) % 768 + 8, :]
        halo = jnp.where(row < 4, right, left)
        for t in range(3):
            tile = t_ref[24 * i + 8 * t : 24 * i + 8 * t + 8, :]
            out_ref[i, 8 * t : 8 * t + 8, :] = jnp.where(lane < 96, tile, roll(halo, 96 - 32 * t, 1))


def add_velocity(old_ref, r_ref, out_ref):
    lane = iota((8, 128), 1)
    row = iota((8, 128), 0)
    col = lane & 15
    slot = lane >> 4
    for i in range(32):
        k = i // 2
        here, depth = r_ref[k, 0:8, :], r_ref[k, 8:16, :]
        if i % 2 == 0:
            other = r_ref[(k - 1) % 16, 0:8, :]
            wide = jnp.where(col == 0, roll(other, -15, 1), roll(here, 1, 1))
            near = here
        else:
            other = r_ref[(k + 1) % 16, 0:8, :]
            wide = jnp.where(col < 9, roll(here, -7, 1), roll(other, 9, 1))
            near = jnp.where(col < 8, roll(here, -8, 1), roll(other, 8, 1))
            depth = jnp.where(col < 8, roll(depth, -8, 1), roll(r_ref[(k + 1) % 16, 8:16, :], 8, 1))
        tile = jnp.where(slot < 4, wide, near)
        tile = jnp.where((slot >= 4) & (col >= 9), roll(depth, 73, 1), tile)
        tile = jnp.where((slot < 2) & (col >= 11), roll(depth, -53, 1), tile)
        tile = jnp.where(((slot >> 1) == 1) & (col >= 11), roll(depth, -26, 1), tile)
        out_ref[i, 24:32, :] = tile
        rest = jnp.where((slot < 4) & ((col == 7) | (col == 8)), depth, 0.0)
        for bit in (4, 2, 1):
            rest = rest + roll(roll(rest, -bit, 0), 2 * bit, 1)
        stash = roll(rest, 3, 0)
        for t in range(3):
            rows = slice(8 * t, 8 * t + 8)
            out_ref[i, rows, :] = jnp.where((row == 3) & (lane >= 96), roll(stash, 96 - 32 * t, 1), old_ref[i, rows, :])


def hat_rows(rows, slot, ring):
    e = iota((rows, 128), 0)
    if ring:
        e = jnp.where(e > 28, e - 32, e) + 3
    lane = iota((rows, 128), 1)
    away = jnp.abs(e - 3 * (lane & 15))
    return jnp.where((lane >> 4) == slot, jnp.maximum(3 - away, 0), 0)


def weights(y_ref, near_ref, near_z_ref, far_ref, far_z_ref):
    odd = odd_device()
    for v in range(6):
        c = iota((256, 128), 0)
        f = iota((256, 128), 1) + 128 * v
        away = jnp.abs(f - 3 * c)
        away = jnp.minimum(away, 768 - away)
        y_ref[:, 128 * v : 128 * v + 128] = jnp.maximum(3 - away, 0).astype(F32).astype(BF16)

    def both(rows):
        return jnp.concatenate(rows, axis=0).astype(F32).astype(BF16)

    sign = 1 - 2 * odd
    for planes, speeds, xy_ref, z_ref in (((0, 1, 2), range(5), near_ref, near_z_ref), ((3,), (3, 4, 5), far_ref, far_z_ref)):
        xy = both([hat_rows(32, p ^ (3 * odd), True) for p in planes] + [hat_rows(24, 4 + (p ^ (3 * odd)), False) for p in planes])
        z = both([hat_rows(24, jnp.where(odd == 1, 5 - p, p), False) * sign for p in speeds])
        xy_ref[:, 0:128] = xy
        xy_ref[:, 128:256] = xy
        z_ref[:, 0:128] = z
        z_ref[:, 128:256] = z


def prepare(v_ref, s_ref, planes_ref, out_ref, y_ref, near_ref, near_z_ref, far_ref, far_z_ref, t_ref):
    pack_velocity(v_ref, planes_ref)
    pack_scalar(s_ref, out_ref, t_ref)
    weights(y_ref, near_ref, near_z_ref, far_ref, far_z_ref)


def two_pieces(x):
    hi = x.astype(BF16)
    return jnp.concatenate([hi, (x - hi.astype(F32)).astype(BF16)], axis=0)


def unpack(s_ref, f_ref, c_ref, planes):
    lane = iota((8, 128), 1)
    row = iota((8, 128), 0)
    col = lane & 15
    slot = lane >> 4
    for i in range(32):
        tiles = [s_ref[i, 8 * t : 8 * t + 8, :] for t in range(3)]
        halo = jnp.where(lane < 32, roll(tiles[0], -96, 1), jnp.where(lane < 64, roll(tiles[1], -64, 1), roll(tiles[2], -32, 1)))
        v, at = divmod(24 * i, 128)
        here = min(24, 128 - at)
        for t, tile in enumerate(tiles + [halo]):
            rows = slice(8 * t, 8 * t + 8)
            for n, p in enumerate(planes):
                moved = roll(tile, at - 24 * p, 1)
                f_ref[n, rows, 128 * v + at : 128 * v + at + here] = moved[:, at : at + here]
                if here < 24:
                    f_ref[n, rows, 128 * v + 128 : 128 * v + 128 + 24 - here] = moved[:, : 24 - here]
        packed = s_ref[i, 24:32, :]
        rest = jnp.broadcast_to(halo[3:4, :], (8, 128))
        for bit in (1, 2, 4):
            rest = jnp.where((row & bit) == 0, rest, roll(rest, -2 * bit, 1))
        depth = jnp.where(slot >= 4, jnp.where(col < 5, roll(packed, 53, 1), roll(packed, 26, 1)), jnp.where(col < 7, roll(packed, -73, 1), rest))
        c_ref[0, 8 * i : 8 * i + 8, :] = packed * (1.0 / 9.0)
        c_ref[1, 8 * i : 8 * i + 8, :] = depth * (1.0 / 9.0)


def refine(coarse, y_ref, hats_ref):
    both = jnp.dot(two_pieces(coarse.T), y_ref[...], preferred_element_type=F32)
    return jnp.dot(hats_ref[...], two_pieces(both[:128] + both[128:]), preferred_element_type=F32)


def plane_sweeps(f_ref, u_ref, x_ref, q_ref, count):
    def along_x(v, carry):
        part = pl.ds(pl.multiple_of(128 * v, 128), 128)
        for p in range(count):
            x_ref[p, :, part] = sweep_ring(f_ref[p, :, part], u_ref[32 * p : 32 * p + 32, part], 0)[:24]
        return carry

    lax.fori_loop(0, 6, along_x, 0)

    def along_y(t, carry):
        for p in range(count):
            rows = pl.ds(pl.multiple_of(8 * t, 8), 8)
            speed = u_ref[pl.ds(pl.multiple_of(32 * count + 24 * p + 8 * t, 8), 8), :]
            q_ref[p, rows, :] = sweep_ring(x_ref[p, rows, :], speed, 1)
        return carry

    lax.fori_loop(0, 3, along_y, 0)


def near_planes(s_ref, y_ref, hats_ref, hats_z_ref, outer_ref, own_ref, inner_ref, f_ref, c_ref, u_ref, w_ref, x_ref, q_ref):
    unpack(s_ref, f_ref, c_ref, (0, 1, 2))
    u_ref[...] = refine(c_ref[0], y_ref, hats_ref)
    w_ref[...] = refine(c_ref[1], y_ref, hats_z_ref)
    plane_sweeps(f_ref, u_ref, x_ref, q_ref, 3)

    def along_z(v, carry):
        part = pl.ds(pl.multiple_of(128 * v, 128), 128)
        for t in range(3):
            rows = slice(8 * t, 8 * t + 8)
            speeds = [w_ref[24 * p + 8 * t : 24 * p + 8 * t + 8, part] for p in range(5)]
            total = {}
            for p in range(3):
                terms = remesh_terms(speeds[p + 1], speeds[p], speeds[p + 2], q_ref[p, rows, part])
                for m, term in terms.items():
                    total[p + m] = total[p + m] + term if p + m in total else term
            for n in range(3):
                outer_ref[n, rows, part] = total[-1 - n]
            for n in range(4):
                own_ref[n, rows, part] = total[n]
            for n in range(2):
                inner_ref[n, rows, part] = total[4 + n]
        return carry

    lax.fori_loop(0, 6, along_z, 0)


def far_plane(s_ref, y_ref, hats_ref, hats_z_ref, some_ref, rest_ref, own_ref, inner_ref, f_ref, c_ref, u_ref, w_ref, x_ref, q_ref):
    unpack(s_ref, f_ref, c_ref, (3,))
    u_ref[...] = refine(c_ref[0], y_ref, hats_ref)
    w_ref[...] = refine(c_ref[1], y_ref, hats_z_ref)
    plane_sweeps(f_ref, u_ref, x_ref, q_ref, 1)

    def along_z(v, carry):
        part = pl.ds(pl.multiple_of(128 * v, 128), 128)
        for t in range(3):
            rows = slice(8 * t, 8 * t + 8)
            before, speed, after = [w_ref[24 * p + 8 * t : 24 * p + 8 * t + 8, part] for p in range(3)]
            terms = remesh_terms(speed, before, after, q_ref[0, rows, part])
            for n in range(4):
                own_ref[n, rows, part] = some_ref[n, rows, part] + terms[n - 3]
            for n in range(2):
                inner_ref[n, rows, part] = rest_ref[n, rows, part] + terms[1 + n]
            inner_ref[2, rows, part] = terms[3]
        return carry

    lax.fori_loop(0, 6, along_z, 0)


def join(own_ref, outer_ref, inner_ref, out_ref):
    flip = odd_device() * 3
    out_ref[0 ^ flip] = own_ref[0] + outer_ref[0]
    out_ref[1 ^ flip] = own_ref[1] + outer_ref[1] + inner_ref[2]
    out_ref[2 ^ flip] = own_ref[2] + outer_ref[2] + inner_ref[1]
    out_ref[3 ^ flip] = own_ref[3] + inner_ref[0]


def kernel(body, *shapes, scratch=(), alias=None, flops=1e7):
    outs = tuple(jax.ShapeDtypeStruct(*(s if isinstance(s[0], tuple) else (s, F32))) for s in shapes)
    return pl.pallas_call(
        body,
        out_shape=outs if len(outs) > 1 else outs[0],
        scratch_shapes=[pltpu.VMEM(s, F32) for s in scratch],
        input_output_aliases=alias or {},
        cost_estimate=pl.CostEstimate(flops=int(flops), transcendentals=0, bytes_accessed=1 << 20),
        compiler_params=pltpu.CompilerParams(vmem_limit_bytes=16 * 1024 * 1024),
    )


def exchange(x, axis):
    return lax.all_to_all(x, axis, split_axis=0, concat_axis=0, tiled=False)


def sweep_scratch(count, speeds):
    return [(count, 32, 768), (2, 256, 128), (56 * count, 768), (24 * speeds, 768), (count, 24, 768), (count, 24, 768)]


def steps(scalar, velocity):
    tables = [(t, BF16) for t in ((256, 768), (168, 256), (120, 256), (56, 256), (72, 256))]
    coarse = jnp.transpose(velocity, (0, 2, 3, 1))
    planes, chunks, y_weights, near, near_z, far, far_z = kernel(prepare, (16, 16, 128), (32, 32, 128), *tables, scratch=[(768, 128)])(coarse, scalar)
    planes = exchange(planes, "gz")
    chunks = exchange(kernel(add_velocity, (32, 32, 128), alias={0: 0})(chunks, planes), "gy")
    outer, own, inner = kernel(near_planes, (3, 24, 768), (4, 24, 768), (2, 24, 768), scratch=sweep_scratch(3, 5))(chunks, y_weights, near, near_z)
    count = lax.axis_size("gz")
    pairs = [(k, k + 1) for k in range(1, count - 1, 2)]
    outer = lax.ppermute(outer, "gz", pairs + [(b, a) for a, b in pairs])
    own, inner = kernel(far_plane, (4, 24, 768), (3, 24, 768), scratch=sweep_scratch(1, 3), flops=1e9)(chunks, y_weights, far, far_z, own, inner)
    pairs = [(k, k + 1) for k in range(0, count, 2)]
    inner = lax.ppermute(inner, "gz", pairs + [(b, a) for a, b in pairs])
    return kernel(join, (4, 24, 768))(own, outer, inner)


def solution(mesh):
    in_specs = (P("gz", "gy", None), P(None, None, "gy", "gz"))
    out_specs = P("gz", "gy", None)
    return jax.shard_map(steps, mesh=mesh, in_specs=in_specs, out_specs=out_specs, check_vma=False)
```

```python
import jax
import jax.numpy as jnp
from jax import lax
from jax.experimental import pallas as pl
from jax.experimental.pallas import tpu as pltpu
from jax.sharding import PartitionSpec as P


F32 = jnp.float32
BF16 = jnp.bfloat16


def iota(shape, dim):
    return lax.broadcasted_iota(jnp.int32, shape, dim)


def remesh_terms(u, before, after, q):
    up = u >= 0.0
    size = jnp.abs(u)
    a = size - (0.5 * size) * (size - jnp.where(up, after, -before))
    b = a - 0.5
    s = b * b
    e1 = (-1.0 / 16.0 * s + 13.0 / 32.0) * s - 25.0 / 256.0
    e2 = (1.0 / 48.0 * s - 5.0 / 96.0) * s + 3.0 / 256.0
    e0 = 0.5 - e1 - e2
    o0 = ((-25.0 / 12.0 * s + 19.0 / 8.0) * s - 281.0 / 192.0) * b
    o1 = ((25.0 / 24.0 * s - 53.0 / 48.0) * s + 27.0 / 128.0) * b
    o2 = ((-5.0 / 24.0 * s + 3.0 / 16.0) * s - 13.0 / 384.0) * b
    at0 = q * (e0 + o0)
    near1, far1 = q * (e0 - o0), q * (e1 + o1)
    near2, far2 = q * (e1 - o1), q * (e2 + o2)
    near3 = q * (e2 - o2)
    zero = jnp.zeros_like(q)
    return {
        0: at0,
        1: jnp.where(up, near1, far1),
        -1: jnp.where(up, far1, near1),
        2: jnp.where(up, near2, far2),
        -2: jnp.where(up, far2, near2),
        3: jnp.where(up, near3, zero),
        -3: jnp.where(up, zero, near3),
    }


def roll(x, shift, axis):
    n = x.shape[axis]
    shift = shift % n
    return x if shift == 0 else pltpu.roll(x, shift, axis)


def sweep_ring(q, u, axis):
    terms = remesh_terms(u, roll(u, 1, axis), roll(u, -1, axis), q)
    total = terms[0]
    for m in (1, -1, 2, -2, 3, -3):
        total = total + roll(terms[m], m, axis)
    return total


def swap_blocks(x):
    row = iota((8, 128), 0)
    block = iota((8, 128), 1) >> 4
    for bit in (1, 2, 4):
        low = (row & bit) == 0
        first = (block & bit) == 0
        upward = roll(roll(x, -bit, 0), 16 * bit, 1)
        downward = roll(roll(x, bit, 0), -16 * bit, 1)
        x = jnp.where(low == first, x, jnp.where(low, upward, downward))
    return x


def pack_velocity(v_ref, after_ref, out_ref):
    lane = iota((8, 128), 1)
    tiles = []
    for c in range(3):
        block = v_ref[c].reshape(128, 64)
        block = jnp.concatenate([block, jnp.zeros((128, 64), F32)], axis=1).T
        tiles.append([swap_blocks(block[8 * n : 8 * n + 8]) for n in range(8)])
    zero = jnp.zeros((8, 128), F32)
    for k in range(16):
        n, odd = divmod(k, 2)
        if odd == 0:
            out_ref[k, 0:8, :] = jnp.where(lane < 64, tiles[0][n], roll(tiles[1][n], 64, 1))
            before = tiles[2][n - 1] if n > 0 else zero
            planes = jnp.where(lane < 16, roll(before, 16, 1), roll(tiles[2][n], 16, 1))
        else:
            out_ref[k, 0:8, :] = jnp.where(lane < 64, roll(tiles[0][n], -64, 1), tiles[1][n])
            after = tiles[2][n + 1] if n < 7 else zero
            planes = jnp.where(lane < 80, roll(tiles[2][n], -48, 1), roll(after, 80, 1))
        out_ref[k, 8:16, :] = jnp.where(lane < 96, planes, zero)


def odd_device():
    return lax.axis_index("gz") & 1


def pack_chunks(s_ref, r_ref, out_ref, t_ref):
    flip = odd_device() * 3
    for v in range(6):
        part = slice(128 * v, 128 * v + 128)
        block = jnp.concatenate([s_ref[p ^ flip, :, part] for p in range(4)] + [jnp.zeros((32, 128), F32)], axis=0)
        t_ref[part, :] = block.T
    shape = (16, 8, 128)
    lane = iota(shape, 2)
    col = lane & 15
    slot = lane >> 4

    def block(x, step):
        return jnp.concatenate([x[step:], x[:step]], axis=0)

    here, depth = r_ref[:, 0:8, :], r_ref[:, 8:16, :]
    wide = jnp.where(col == 0, block(roll(here, -15, 2), -1), roll(here, 1, 2))
    even = (wide, here, depth)
    wide = jnp.where(col < 9, roll(here, -7, 2), block(roll(here, 9, 2), 1))
    near = jnp.where(col < 8, roll(here, -8, 2), block(roll(here, 8, 2), 1))
    depth = jnp.where(col < 8, roll(depth, -8, 2), block(roll(depth, 8, 2), 1))
    stash = []
    for parity, (wide, near, depth) in enumerate((even, (wide, near, depth))):
        tile = jnp.where(slot < 4, wide, near)
        tile = jnp.where((slot >= 4) & (col >= 9), roll(depth, 73, 2), tile)
        tile = jnp.where((slot < 2) & (col >= 11), roll(depth, -53, 2), tile)
        tile = jnp.where(((slot >> 1) == 1) & (col >= 11), roll(depth, -26, 2), tile)
        rest = jnp.where((slot < 4) & ((col == 7) | (col == 8)), depth, 0.0)
        for bit in (4, 2, 1):
            rest = rest + roll(roll(rest, -bit, 1), 2 * bit, 2)
        stash.append(roll(rest, 3, 1))
        for n in range(16):
            out_ref[2 * n + parity, 24:32, :] = tile[n]
    lane = iota((8, 128), 1)
    row = iota((8, 128), 0)
    for i in range(32):
        left = t_ref[(24 * i - 8) % 768 : (24 * i - 8) % 768 + 8, :]
        right = t_ref[(24 * i + 24) % 768 : (24 * i + 24) % 768 + 8, :]
        halo = jnp.where(row < 3, right, jnp.where(row == 3, stash[i % 2][i // 2], left))
        for t in range(3):
            tile = t_ref[24 * i + 8 * t : 24 * i + 8 * t + 8, :]
            out_ref[i, 8 * t : 8 * t + 8, :] = jnp.where(lane < 96, tile, roll(halo, 96 - 32 * t, 1))


def hat_rows(rows, slot, ring):
    e = iota((rows, 128), 0)
    if ring:
        e = jnp.where(e > 28, e - 32, e) + 3
    lane = iota((rows, 128), 1)
    away = jnp.abs(e - 3 * (lane & 15))
    return jnp.where((lane >> 4) == slot, jnp.maximum(3 - away, 0), 0)


def weights(y_ref, near_ref, near_z_ref, far_ref, far_z_ref):
    odd = odd_device()
    for v in range(6):
        c = iota((256, 128), 0)
        f = iota((256, 128), 1) + 128 * v
        away = jnp.abs(f - 3 * c)
        away = jnp.minimum(away, 768 - away)
        y_ref[:, 128 * v : 128 * v + 128] = jnp.maximum(3 - away, 0).astype(F32).astype(BF16)

    def both(rows):
        return jnp.concatenate(rows, axis=0).astype(F32).astype(BF16)

    sign = 1 - 2 * odd
    for planes, speeds, xy_ref, z_ref in (((0, 1, 2), range(5), near_ref, near_z_ref), ((3,), (3, 4, 5), far_ref, far_z_ref)):
        xy = both([hat_rows(32, p ^ (3 * odd), True) for p in planes] + [hat_rows(24, 4 + (p ^ (3 * odd)), False) for p in planes])
        z = both([hat_rows(24, jnp.where(odd == 1, 5 - p, p), False) * sign for p in speeds])
        xy_ref[:, 0:128] = xy
        xy_ref[:, 128:256] = xy
        z_ref[:, 0:128] = z
        z_ref[:, 128:256] = z


def two_pieces(x):
    hi = x.astype(BF16)
    return jnp.concatenate([hi, (x - hi.astype(F32)).astype(BF16)], axis=0)


def unpack(s_ref, f_ref, c_ref, h_ref, planes):
    shape = (32, 8, 128)
    lane = iota(shape, 2)
    row = iota(shape, 1)
    col = lane & 15
    slot = lane >> 4
    parts = [roll(s_ref[:, 8 * t : 8 * t + 8, :], 32 * t - 96, 2) for t in range(3)]
    halo = jnp.where(lane < 32, parts[0], jnp.where(lane < 64, parts[1], parts[2]))
    h_ref[...] = halo
    packed = s_ref[:, 24:32, :]
    c_ref[0] = packed.reshape(256, 128) * (1.0 / 9.0)
    rest = jnp.broadcast_to(halo[:, 3:4, :], shape)
    for bit in (1, 2, 4):
        rest = jnp.where((row & bit) == 0, rest, roll(rest, -2 * bit, 2))
    depth = jnp.where(slot >= 4, jnp.where(col < 5, roll(packed, 53, 2), roll(packed, 26, 2)), jnp.where(col < 7, roll(packed, -73, 2), rest))
    c_ref[1] = depth.reshape(256, 128) * (1.0 / 9.0)
    for i in range(32):
        whole = jnp.concatenate([s_ref[i, 0:24, :], h_ref[i]], axis=0)
        v, at = divmod(24 * i, 128)
        here = min(24, 128 - at)
        for n, p in enumerate(planes):
            moved = roll(whole, at - 24 * p, 1)
            f_ref[n, :, 128 * v + at : 128 * v + at + here] = moved[:, at : at + here]
            if here < 24:
                f_ref[n, :, 128 * v + 128 : 128 * v + 128 + 24 - here] = moved[:, : 24 - here]


def refine(coarse, y_ref, hats_ref):
    both = jnp.dot(two_pieces(coarse.T), y_ref[...], preferred_element_type=F32)
    return jnp.dot(hats_ref[...], two_pieces(both[:128] + both[128:]), preferred_element_type=F32)


def plane_sweeps(f_ref, u_ref, x_ref, q_ref, count):
    def along_x(v, carry):
        part = pl.ds(pl.multiple_of(128 * v, 128), 128)
        for p in range(count):
            x_ref[p, :, part] = sweep_ring(f_ref[p, :, part], u_ref[32 * p : 32 * p + 32, part], 0)[:24]
        return carry

    lax.fori_loop(0, 6, along_x, 0)

    def along_y(t, carry):
        for p in range(count):
            rows = pl.ds(pl.multiple_of(8 * t, 8), 8)
            speed = u_ref[pl.ds(pl.multiple_of(32 * count + 24 * p + 8 * t, 8), 8), :]
            q_ref[p, rows, :] = sweep_ring(x_ref[p, rows, :], speed, 1)
        return carry

    lax.fori_loop(0, 3, along_y, 0)


def near_planes(s_ref, y_ref, hats_ref, hats_z_ref, outer_ref, own_ref, inner_ref, f_ref, c_ref, h_ref, u_ref, w_ref, x_ref, q_ref):
    unpack(s_ref, f_ref, c_ref, h_ref, (0, 1, 2))
    u_ref[...] = refine(c_ref[0], y_ref, hats_ref)
    w_ref[...] = refine(c_ref[1], y_ref, hats_z_ref)
    plane_sweeps(f_ref, u_ref, x_ref, q_ref, 3)

    def along_z(v, carry):
        part = pl.ds(pl.multiple_of(128 * v, 128), 128)
        for t in range(3):
            rows = slice(8 * t, 8 * t + 8)
            speeds = [w_ref[24 * p + 8 * t : 24 * p + 8 * t + 8, part] for p in range(5)]
            total = {}
            for p in range(3):
                terms = remesh_terms(speeds[p + 1], speeds[p], speeds[p + 2], q_ref[p, rows, part])
                for m, term in terms.items():
                    total[p + m] = total[p + m] + term if p + m in total else term
            for n in range(3):
                outer_ref[n, rows, part] = total[-1 - n]
            for n in range(4):
                own_ref[n, rows, part] = total[n]
            for n in range(2):
                inner_ref[n, rows, part] = total[4 + n]
        return carry

    lax.fori_loop(0, 6, along_z, 0)


def far_plane(s_ref, y_ref, hats_ref, hats_z_ref, some_ref, rest_ref, own_ref, inner_ref, f_ref, c_ref, h_ref, u_ref, w_ref, x_ref, q_ref):
    unpack(s_ref, f_ref, c_ref, h_ref, (3,))
    u_ref[...] = refine(c_ref[0], y_ref, hats_ref)
    w_ref[...] = refine(c_ref[1], y_ref, hats_z_ref)
    plane_sweeps(f_ref, u_ref, x_ref, q_ref, 1)

    def along_z(v, carry):
        part = pl.ds(pl.multiple_of(128 * v, 128), 128)
        for t in range(3):
            rows = slice(8 * t, 8 * t + 8)
            before, speed, after = [w_ref[24 * p + 8 * t : 24 * p + 8 * t + 8, part] for p in range(3)]
            terms = remesh_terms(speed, before, after, q_ref[0, rows, part])
            for n in range(4):
                own_ref[n, rows, part] = some_ref[n, rows, part] + terms[n - 3]
            for n in range(2):
                inner_ref[n, rows, part] = rest_ref[n, rows, part] + terms[1 + n]
            inner_ref[2, rows, part] = terms[3]
        return carry

    lax.fori_loop(0, 6, along_z, 0)


def join(own_ref, outer_ref, inner_ref, out_ref):
    flip = odd_device() * 3
    out_ref[0 ^ flip] = own_ref[0] + outer_ref[0]
    out_ref[1 ^ flip] = own_ref[1] + outer_ref[1] + inner_ref[2]
    out_ref[2 ^ flip] = own_ref[2] + outer_ref[2] + inner_ref[1]
    out_ref[3 ^ flip] = own_ref[3] + inner_ref[0]


def kernel(body, *shapes, scratch=(), flops=1e7, specs=None):
    outs = tuple(jax.ShapeDtypeStruct(*(s if isinstance(s[0], tuple) else (s, F32))) for s in shapes)
    extra = {"in_specs": [pl.BlockSpec(memory_space=m) for m in specs]} if specs else {}
    return pl.pallas_call(
        body,
        out_shape=outs if len(outs) > 1 else outs[0],
        scratch_shapes=[pltpu.VMEM(s, F32) for s in scratch],
        cost_estimate=pl.CostEstimate(flops=int(flops), transcendentals=0, bytes_accessed=1 << 20),
        compiler_params=pltpu.CompilerParams(vmem_limit_bytes=16 * 1024 * 1024),
        **extra,
    )


def exchange(x, axis):
    return lax.all_to_all(x, axis, split_axis=0, concat_axis=0, tiled=False)


def sweep_scratch(count, speeds):
    return [(count, 32, 768), (2, 256, 128), (32, 8, 128), (56 * count, 768), (24 * speeds, 768), (count, 24, 768), (count, 24, 768)]


def steps(scalar, velocity):
    tables = [(t, BF16) for t in ((256, 768), (168, 256), (120, 256), (56, 256), (72, 256))]
    y_weights, near, near_z, far, far_z = kernel(weights, *tables)()
    coarse = jnp.transpose(velocity, (0, 2, 3, 1))
    planes = exchange(kernel(pack_velocity, (16, 16, 128), specs=(pltpu.VMEM, pl.ANY))(coarse, near), "gz")
    chunks = exchange(kernel(pack_chunks, (32, 32, 128), scratch=[(768, 128)])(scalar, planes), "gy")
    outer, own, inner = kernel(near_planes, (3, 24, 768), (4, 24, 768), (2, 24, 768), scratch=sweep_scratch(3, 5))(chunks, y_weights, near, near_z)
    count = lax.axis_size("gz")
    pairs = [(k, k + 1) for k in range(1, count - 1, 2)]
    outer = lax.ppermute(outer, "gz", pairs + [(b, a) for a, b in pairs])
    own, inner = kernel(far_plane, (4, 24, 768), (3, 24, 768), scratch=sweep_scratch(1, 3), flops=1e9)(chunks, y_weights, far, far_z, own, inner)
    pairs = [(k, k + 1) for k in range(0, count, 2)]
    inner = lax.ppermute(inner, "gz", pairs + [(b, a) for a, b in pairs])
    return kernel(join, (4, 24, 768))(own, outer, inner)


def solution(mesh):
    in_specs = (P("gz", "gy", None), P(None, None, "gy", "gz"))
    out_specs = P("gz", "gy", None)
    return jax.shard_map(steps, mesh=mesh, in_specs=in_specs, out_specs=out_specs, check_vma=False)
```

```python
import jax
import jax.numpy as jnp
from jax import lax
from jax.experimental import pallas as pl
from jax.experimental.pallas import tpu as pltpu
from jax.sharding import PartitionSpec as P


F32 = jnp.float32
BF16 = jnp.bfloat16


def iota(shape, dim):
    return lax.broadcasted_iota(jnp.int32, shape, dim)


def remesh_terms(u, before, after, q):
    up = u >= 0.0
    size = jnp.abs(u)
    a = size - (0.5 * size) * (size - jnp.where(up, after, -before))
    b = a - 0.5
    s = b * b
    g1, g3, g5 = s - 0.25, s - 2.25, s - 6.25
    e2 = g1 * g3
    e1 = (g1 * g5) * -3.0
    e0 = (g3 * g5) * 2.0
    g = g1 * b
    o2 = g * (6.5 - 10.0 * s)
    o1 = g * (50.0 * s - 40.5)
    o0 = g * (89.0 - 100.0 * s) - 48.0 * b
    q = q * (1.0 / 48.0)
    at0 = q * (e0 + o0)
    near1, far1 = q * (e0 - o0), q * (e1 + o1)
    near2, far2 = q * (e1 - o1), q * (e2 + o2)
    near3 = q * (e2 - o2)
    zero = jnp.zeros_like(q)
    return {
        0: at0,
        1: jnp.where(up, near1, far1),
        -1: jnp.where(up, far1, near1),
        2: jnp.where(up, near2, far2),
        -2: jnp.where(up, far2, near2),
        3: jnp.where(up, near3, zero),
        -3: jnp.where(up, zero, near3),
    }


def roll(x, shift, axis):
    n = x.shape[axis]
    shift = shift % n
    return x if shift == 0 else pltpu.roll(x, shift, axis)


def sweep_ring(q, u, axis):
    terms = remesh_terms(u, roll(u, 1, axis), roll(u, -1, axis), q)
    total = terms[0]
    for m in (1, -1, 2, -2, 3, -3):
        total = total + roll(terms[m], m, axis)
    return total


def swap_blocks(x):
    row = iota((8, 128), 0)
    block = iota((8, 128), 1) >> 4
    for bit in (1, 2, 4):
        low = (row & bit) == 0
        first = (block & bit) == 0
        upward = roll(roll(x, -bit, 0), 16 * bit, 1)
        downward = roll(roll(x, bit, 0), -16 * bit, 1)
        x = jnp.where(low == first, x, jnp.where(low, upward, downward))
    return x


def pack_velocity(v_ref, after_ref, out_ref):
    lane = iota((8, 128), 1)
    tiles = []
    for c in range(3):
        block = v_ref[c].reshape(128, 64)
        block = jnp.concatenate([block, jnp.zeros((128, 64), F32)], axis=1).T
        tiles.append([swap_blocks(block[8 * n : 8 * n + 8]) for n in range(8)])
    zero = jnp.zeros((8, 128), F32)
    for k in range(16):
        n, odd = divmod(k, 2)
        if odd == 0:
            out_ref[k, 0:8, :] = jnp.where(lane < 64, tiles[0][n], roll(tiles[1][n], 64, 1))
            before = tiles[2][n - 1] if n > 0 else zero
            planes = jnp.where(lane < 16, roll(before, 16, 1), roll(tiles[2][n], 16, 1))
        else:
            out_ref[k, 0:8, :] = jnp.where(lane < 64, roll(tiles[0][n], -64, 1), tiles[1][n])
            after = tiles[2][n + 1] if n < 7 else zero
            planes = jnp.where(lane < 80, roll(tiles[2][n], -48, 1), roll(after, 80, 1))
        out_ref[k, 8:16, :] = jnp.where(lane < 96, planes, zero)


def odd_device():
    return lax.axis_index("gz") & 1


def pack_chunks(s_ref, r_ref, out_ref, t_ref):
    flip = odd_device() * 3
    for v in range(6):
        part = slice(128 * v, 128 * v + 128)
        block = jnp.concatenate([s_ref[p ^ flip, :, part] for p in range(4)] + [jnp.zeros((32, 128), F32)], axis=0)
        t_ref[part, :] = block.T
    shape = (16, 8, 128)
    lane = iota(shape, 2)
    col = lane & 15
    slot = lane >> 4

    def block(x, step):
        return jnp.concatenate([x[step:], x[:step]], axis=0)

    here, depth = r_ref[:, 0:8, :], r_ref[:, 8:16, :]
    wide = jnp.where(col == 0, block(roll(here, -15, 2), -1), roll(here, 1, 2))
    even = (wide, here, depth)
    wide = jnp.where(col < 9, roll(here, -7, 2), block(roll(here, 9, 2), 1))
    near = jnp.where(col < 8, roll(here, -8, 2), block(roll(here, 8, 2), 1))
    depth = jnp.where(col < 8, roll(depth, -8, 2), block(roll(depth, 8, 2), 1))
    stash = []
    for parity, (wide, near, depth) in enumerate((even, (wide, near, depth))):
        tile = jnp.where(slot < 4, wide, near)
        tile = jnp.where((slot >= 4) & (col >= 9), roll(depth, 73, 2), tile)
        tile = jnp.where((slot < 2) & (col >= 11), roll(depth, -53, 2), tile)
        tile = jnp.where(((slot >> 1) == 1) & (col >= 11), roll(depth, -26, 2), tile)
        rest = jnp.where((slot < 4) & ((col == 7) | (col == 8)), depth, 0.0)
        for bit in (4, 2, 1):
            rest = rest + roll(roll(rest, -bit, 1), 2 * bit, 2)
        stash.append(roll(rest, 3, 1))
        for n in range(16):
            out_ref[2 * n + parity, 24:32, :] = tile[n]
    lane = iota((8, 128), 1)
    row = iota((8, 128), 0)
    for i in range(32):
        left = t_ref[(24 * i - 8) % 768 : (24 * i - 8) % 768 + 8, :]
        right = t_ref[(24 * i + 24) % 768 : (24 * i + 24) % 768 + 8, :]
        halo = jnp.where(row < 3, right, jnp.where(row == 3, stash[i % 2][i // 2], left))
        for t in range(3):
            tile = t_ref[24 * i + 8 * t : 24 * i + 8 * t + 8, :]
            out_ref[i, 8 * t : 8 * t + 8, :] = jnp.where(lane < 96, tile, roll(halo, 96 - 32 * t, 1))


def hat_rows(rows, slot, ring):
    e = iota((rows, 128), 0)
    if ring:
        e = jnp.where(e > 28, e - 32, e) + 3
    lane = iota((rows, 128), 1)
    away = jnp.abs(e - 3 * (lane & 15))
    return jnp.where((lane >> 4) == slot, jnp.maximum(3 - away, 0), 0)


def weights(y_ref, near_ref, near_z_ref, far_ref, far_z_ref):
    odd = odd_device()
    for v in range(6):
        c = iota((256, 128), 0)
        f = iota((256, 128), 1) + 128 * v
        away = jnp.abs(f - 3 * c)
        away = jnp.minimum(away, 768 - away)
        y_ref[:, 128 * v : 128 * v + 128] = jnp.maximum(3 - away, 0).astype(F32).astype(BF16)

    def both(rows):
        return jnp.concatenate(rows, axis=0).astype(F32).astype(BF16)

    sign = 1 - 2 * odd
    for planes, speeds, xy_ref, z_ref in (((0, 1, 2), range(5), near_ref, near_z_ref), ((3,), range(6), far_ref, far_z_ref)):
        xy = both([hat_rows(32, p ^ (3 * odd), True) for p in planes] + [hat_rows(24, 4 + (p ^ (3 * odd)), False) for p in planes])
        z = both([hat_rows(24, jnp.where(odd == 1, 5 - p, p), False) * sign for p in speeds])
        xy_ref[:, 0:128] = xy
        xy_ref[:, 128:256] = xy
        z_ref[:, 0:128] = z
        z_ref[:, 128:256] = z


def two_pieces(x):
    hi = x.astype(BF16)
    return jnp.concatenate([hi, (x - hi.astype(F32)).astype(BF16)], axis=0)


def unpack(s_ref, f_ref, c_ref, h_ref, planes):
    shape = (32, 8, 128)
    lane = iota(shape, 2)
    row = iota(shape, 1)
    col = lane & 15
    slot = lane >> 4
    parts = [roll(s_ref[:, 8 * t : 8 * t + 8, :], 32 * t - 96, 2) for t in range(3)]
    halo = jnp.where(lane < 32, parts[0], jnp.where(lane < 64, parts[1], parts[2]))
    h_ref[...] = halo
    packed = s_ref[:, 24:32, :]
    c_ref[0] = packed.reshape(256, 128) * (1.0 / 9.0)
    rest = jnp.broadcast_to(halo[:, 3:4, :], shape)
    for bit in (1, 2, 4):
        rest = jnp.where((row & bit) == 0, rest, roll(rest, -2 * bit, 2))
    depth = jnp.where(slot >= 4, jnp.where(col < 5, roll(packed, 53, 2), roll(packed, 26, 2)), jnp.where(col < 7, roll(packed, -73, 2), rest))
    c_ref[1] = depth.reshape(256, 128) * (1.0 / 9.0)
    for i in range(32):
        whole = jnp.concatenate([s_ref[i, 0:24, :], h_ref[i]], axis=0)
        v, at = divmod(24 * i, 128)
        here = min(24, 128 - at)
        for n, p in enumerate(planes):
            moved = roll(whole, at - 24 * p, 1)
            f_ref[n, :, 128 * v + at : 128 * v + at + here] = moved[:, at : at + here]
            if here < 24:
                f_ref[n, :, 128 * v + 128 : 128 * v + 128 + 24 - here] = moved[:, : 24 - here]


def refine(coarse, y_ref, hats_ref):
    both = jnp.dot(two_pieces(coarse.T), y_ref[...], preferred_element_type=F32)
    return jnp.dot(hats_ref[...], two_pieces(both[:128] + both[128:]), preferred_element_type=F32)


def plane_sweeps(f_ref, u_ref, x_ref, q_ref, count):
    def along_x(v, carry):
        part = pl.ds(pl.multiple_of(128 * v, 128), 128)
        for p in range(count):
            x_ref[p, :, part] = sweep_ring(f_ref[p, :, part], u_ref[32 * p : 32 * p + 32, part], 0)[:24]
        return carry

    lax.fori_loop(0, 6, along_x, 0)

    def along_y(t, carry):
        for p in range(count):
            rows = pl.ds(pl.multiple_of(8 * t, 8), 8)
            speed = u_ref[pl.ds(pl.multiple_of(32 * count + 24 * p + 8 * t, 8), 8), :]
            q_ref[p, rows, :] = sweep_ring(x_ref[p, rows, :], speed, 1)
        return carry

    lax.fori_loop(0, 3, along_y, 0)


def near_planes(s_ref, y_ref, hats_ref, hats_z_ref, outer_ref, q_ref, f_ref, c_ref, h_ref, u_ref, w_ref, x_ref):
    unpack(s_ref, f_ref, c_ref, h_ref, (0, 1, 2))
    u_ref[...] = refine(c_ref[0], y_ref, hats_ref)
    w_ref[...] = refine(c_ref[1], y_ref, hats_z_ref)
    plane_sweeps(f_ref, u_ref, x_ref, q_ref, 3)

    def along_z(v, carry):
        part = pl.ds(pl.multiple_of(128 * v, 128), 128)
        for t in range(3):
            rows = slice(8 * t, 8 * t + 8)
            speeds = [w_ref[24 * p + 8 * t : 24 * p + 8 * t + 8, part] for p in range(5)]
            first, second, third = [remesh_terms(speeds[p + 1], speeds[p], speeds[p + 2], q_ref[p, rows, part]) for p in range(3)]
            outer_ref[0, rows, part] = first[-1] + second[-2] + third[-3]
            outer_ref[1, rows, part] = first[-2] + second[-3]
            outer_ref[2, rows, part] = first[-3]
        return carry

    lax.fori_loop(0, 6, along_z, 0)


def far_plane(s_ref, y_ref, hats_ref, hats_z_ref, near_ref, own_ref, inner_ref, f_ref, c_ref, h_ref, u_ref, w_ref, x_ref, q_ref):
    unpack(s_ref, f_ref, c_ref, h_ref, (3,))
    u_ref[...] = refine(c_ref[0], y_ref, hats_ref)
    w_ref[...] = refine(c_ref[1], y_ref, hats_z_ref)
    plane_sweeps(f_ref, u_ref, x_ref, q_ref, 1)

    def along_z(v, carry):
        part = pl.ds(pl.multiple_of(128 * v, 128), 128)
        for t in range(3):
            rows = slice(8 * t, 8 * t + 8)
            speeds = [w_ref[24 * p + 8 * t : 24 * p + 8 * t + 8, part] for p in range(6)]
            total = {}
            for p in range(4):
                q = q_ref[0, rows, part] if p == 3 else near_ref[p, rows, part]
                terms = remesh_terms(speeds[p + 1], speeds[p], speeds[p + 2], q)
                for m, term in terms.items():
                    total[p + m] = total[p + m] + term if p + m in total else term
            for n in range(4):
                own_ref[n, rows, part] = total[n]
            for n in range(3):
                inner_ref[n, rows, part] = total[4 + n]
        return carry

    lax.fori_loop(0, 6, along_z, 0)


def join(own_ref, outer_ref, inner_ref, out_ref):
    flip = odd_device() * 3
    out_ref[0 ^ flip] = own_ref[0] + outer_ref[0]
    out_ref[1 ^ flip] = own_ref[1] + outer_ref[1] + inner_ref[2]
    out_ref[2 ^ flip] = own_ref[2] + outer_ref[2] + inner_ref[1]
    out_ref[3 ^ flip] = own_ref[3] + inner_ref[0]


def kernel(body, *shapes, scratch=(), flops=1e7, specs=None):
    outs = tuple(jax.ShapeDtypeStruct(*(s if isinstance(s[0], tuple) else (s, F32))) for s in shapes)
    extra = {"in_specs": [pl.BlockSpec(memory_space=m) for m in specs]} if specs else {}
    return pl.pallas_call(
        body,
        out_shape=outs if len(outs) > 1 else outs[0],
        scratch_shapes=[pltpu.VMEM(s, F32) for s in scratch],
        cost_estimate=pl.CostEstimate(flops=int(flops), transcendentals=0, bytes_accessed=1 << 20),
        compiler_params=pltpu.CompilerParams(vmem_limit_bytes=16 * 1024 * 1024),
        **extra,
    )


def exchange(x, axis):
    return lax.all_to_all(x, axis, split_axis=0, concat_axis=0, tiled=False)


def sweep_scratch(count, speeds):
    return [(count, 32, 768), (2, 256, 128), (32, 8, 128), (56 * count, 768), (24 * speeds, 768), (count, 24, 768)]


def steps(scalar, velocity):
    tables = [(t, BF16) for t in ((256, 768), (168, 256), (120, 256), (56, 256), (144, 256))]
    y_weights, near, near_z, far, far_z = kernel(weights, *tables, flops=1e9)()
    coarse = jnp.transpose(velocity, (0, 2, 3, 1))
    planes = exchange(kernel(pack_velocity, (16, 16, 128), specs=(pltpu.VMEM, pl.ANY))(coarse, near), "gz")
    chunks = exchange(kernel(pack_chunks, (32, 32, 128), scratch=[(768, 128)])(scalar, planes), "gy")
    outer, swept = kernel(near_planes, (3, 24, 768), (3, 24, 768), scratch=sweep_scratch(3, 5))(chunks, y_weights, near, near_z)
    count = lax.axis_size("gz")
    pairs = [(k, k + 1) for k in range(1, count - 1, 2)]
    outer = lax.ppermute(outer, "gz", pairs + [(b, a) for a, b in pairs])
    own, inner = kernel(far_plane, (4, 24, 768), (3, 24, 768), scratch=sweep_scratch(1, 6) + [(1, 24, 768)], flops=1e9)(chunks, y_weights, far, far_z, swept)
    pairs = [(k, k + 1) for k in range(0, count, 2)]
    inner = lax.ppermute(inner, "gz", pairs + [(b, a) for a, b in pairs])
    return kernel(join, (4, 24, 768))(own, outer, inner)


def solution(mesh):
    in_specs = (P("gz", "gy", None), P(None, None, "gy", "gz"))
    out_specs = P("gz", "gy", None)
    return jax.shard_map(steps, mesh=mesh, in_specs=in_specs, out_specs=out_specs, check_vma=False)
```

```python
import jax
import jax.numpy as jnp
from jax import lax
from jax.experimental import pallas as pl
from jax.experimental.pallas import tpu as pltpu
from jax.sharding import PartitionSpec as P


F32 = jnp.float32
BF16 = jnp.bfloat16


def iota(shape, dim):
    return lax.broadcasted_iota(jnp.int32, shape, dim)


def remesh_terms(h, before, after, q):
    up = h >= 0.0
    b = jnp.abs(h - jnp.abs(h) * (h - jnp.where(up, after, before))) - 0.25
    s = b * b
    g1, g3, g5 = s - 1.0 / 16.0, s - 9.0 / 16.0, s - 25.0 / 16.0
    e2 = g1 * g3
    e1 = (g1 * g5) * -3.0
    e0 = (g3 * g5) * 2.0
    g = g1 * b
    o2 = g * (3.25 - 20.0 * s)
    o1 = g * (100.0 * s - 20.25)
    o0 = g * (44.5 - 200.0 * s) - 6.0 * b
    at0 = q * (e0 + o0)
    near1, far1 = q * (e0 - o0), q * (e1 + o1)
    near2, far2 = q * (e1 - o1), q * (e2 + o2)
    near3 = q * (e2 - o2)
    zero = jnp.zeros_like(q)
    return {
        0: at0,
        1: jnp.where(up, near1, far1),
        -1: jnp.where(up, far1, near1),
        2: jnp.where(up, near2, far2),
        -2: jnp.where(up, far2, near2),
        3: jnp.where(up, near3, zero),
        -3: jnp.where(up, zero, near3),
    }


def roll(x, shift, axis):
    n = x.shape[axis]
    shift = shift % n
    return x if shift == 0 else pltpu.roll(x, shift, axis)


def sweep_ring(q, u, axis):
    terms = remesh_terms(u, roll(u, 1, axis), roll(u, -1, axis), q)
    total = terms[0]
    for m in (1, -1, 2, -2, 3, -3):
        total = total + roll(terms[m], m, axis)
    return total


def swap_blocks(x):
    row = iota((8, 128), 0)
    block = iota((8, 128), 1) >> 4
    for bit in (1, 2, 4):
        low = (row & bit) == 0
        first = (block & bit) == 0
        upward = roll(roll(x, -bit, 0), 16 * bit, 1)
        downward = roll(roll(x, bit, 0), -16 * bit, 1)
        x = jnp.where(low == first, x, jnp.where(low, upward, downward))
    return x


def pack_velocity(v_ref, after_ref, out_ref):
    lane = iota((8, 128), 1)
    tiles = []
    for c in range(3):
        block = v_ref[c].reshape(128, 64)
        block = jnp.concatenate([block, jnp.zeros((128, 64), F32)], axis=1).T
        tiles.append([swap_blocks(block[8 * n : 8 * n + 8]) for n in range(8)])
    zero = jnp.zeros((8, 128), F32)
    for k in range(16):
        n, odd = divmod(k, 2)
        if odd == 0:
            out_ref[k, 0:8, :] = jnp.where(lane < 64, tiles[0][n], roll(tiles[1][n], 64, 1))
            before = tiles[2][n - 1] if n > 0 else zero
            planes = jnp.where(lane < 16, roll(before, 16, 1), roll(tiles[2][n], 16, 1))
        else:
            out_ref[k, 0:8, :] = jnp.where(lane < 64, roll(tiles[0][n], -64, 1), tiles[1][n])
            after = tiles[2][n + 1] if n < 7 else zero
            planes = jnp.where(lane < 80, roll(tiles[2][n], -48, 1), roll(after, 80, 1))
        out_ref[k, 8:16, :] = jnp.where(lane < 96, planes, zero)


def odd_device():
    return lax.axis_index("gz") & 1


def pack_chunks(s_ref, r_ref, out_ref, t_ref):
    flip = odd_device() * 3
    for v in range(6):
        part = slice(128 * v, 128 * v + 128)
        block = jnp.concatenate([s_ref[p ^ flip, :, part] for p in range(4)] + [jnp.zeros((32, 128), F32)], axis=0)
        t_ref[part, :] = block.T
    shape = (16, 8, 128)
    lane = iota(shape, 2)
    col = lane & 15
    slot = lane >> 4

    def block(x, step):
        return jnp.concatenate([x[step:], x[:step]], axis=0)

    here, depth = r_ref[:, 0:8, :], r_ref[:, 8:16, :]
    wide = jnp.where(col == 0, block(roll(here, -15, 2), -1), roll(here, 1, 2))
    even = (wide, here, depth)
    wide = jnp.where(col < 9, roll(here, -7, 2), block(roll(here, 9, 2), 1))
    near = jnp.where(col < 8, roll(here, -8, 2), block(roll(here, 8, 2), 1))
    depth = jnp.where(col < 8, roll(depth, -8, 2), block(roll(depth, 8, 2), 1))
    stash = []
    for parity, (wide, near, depth) in enumerate((even, (wide, near, depth))):
        tile = jnp.where(slot < 4, wide, near)
        tile = jnp.where((slot >= 4) & (col >= 9), roll(depth, 73, 2), tile)
        tile = jnp.where((slot < 2) & (col >= 11), roll(depth, -53, 2), tile)
        tile = jnp.where(((slot >> 1) == 1) & (col >= 11), roll(depth, -26, 2), tile)
        rest = jnp.where((slot < 4) & ((col == 7) | (col == 8)), depth, 0.0)
        for bit in (4, 2, 1):
            rest = rest + roll(roll(rest, -bit, 1), -2 * bit, 2)
        stash.append(roll(roll(rest, 3, 1), 16, 2))
        for n in range(16):
            out_ref[2 * n + parity, 24:32, :] = tile[n]
    lane = iota((8, 128), 1)
    row = iota((8, 128), 0)
    for i in range(32):
        left = t_ref[(24 * i - 8) % 768 : (24 * i - 8) % 768 + 8, :]
        right = t_ref[(24 * i + 24) % 768 : (24 * i + 24) % 768 + 8, :]
        halo = jnp.where(row < 3, right, jnp.where(row == 3, stash[i % 2][i // 2], left))
        for t in range(3):
            tile = t_ref[24 * i + 8 * t : 24 * i + 8 * t + 8, :]
            out_ref[i, 8 * t : 8 * t + 8, :] = jnp.where(lane < 96, tile, roll(halo, 96 - 32 * t, 1))


def hat_rows(rows, slot, ring):
    e = iota((rows, 128), 0)
    if ring:
        e = jnp.where(e > 28, e - 32, e) + 3
    lane = iota((rows, 128), 1)
    away = jnp.abs(e - 3 * (lane & 15))
    return jnp.where((lane >> 4) == slot, jnp.maximum(3 - away, 0), 0)


def weights(y_ref, near_ref, near_z_ref, far_ref, far_z_ref):
    odd = odd_device()
    for v in range(6):
        c = iota((256, 128), 0)
        f = iota((256, 128), 1) + 128 * v
        away = jnp.abs(f - 3 * c)
        away = jnp.minimum(away, 768 - away)
        y_ref[:, 128 * v : 128 * v + 128] = jnp.maximum(3 - away, 0).astype(F32).astype(BF16)

    def both(rows):
        return jnp.concatenate(rows, axis=0).astype(F32).astype(BF16)

    sign = 1 - 2 * odd
    for planes, speeds, xy_ref, z_ref in (((0, 1, 2), range(5), near_ref, near_z_ref), ((3,), range(6), far_ref, far_z_ref)):
        xy = both([hat_rows(32, p ^ (3 * odd), True) for p in planes] + [hat_rows(24, 4 + (p ^ (3 * odd)), False) for p in planes])
        z = both([hat_rows(24, jnp.where(odd == 1, 5 - p, p), False) * sign for p in speeds])
        xy_ref[:, 0:128] = xy
        xy_ref[:, 128:256] = xy
        z_ref[:, 0:128] = z
        z_ref[:, 128:256] = z


def two_pieces(x):
    hi = x.astype(BF16)
    return jnp.concatenate([hi, (x - hi.astype(F32)).astype(BF16)], axis=0)


def unpack(s_ref, f_ref, c_ref, h_ref, planes):
    shape = (32, 8, 128)
    lane = iota(shape, 2)
    row = iota(shape, 1)
    col = lane & 15
    slot = lane >> 4
    parts = [roll(s_ref[:, 8 * t : 8 * t + 8, :], 32 * t - 96, 2) for t in range(3)]
    halo = jnp.where(lane < 32, parts[0], jnp.where(lane < 64, parts[1], parts[2]))
    h_ref[...] = halo
    packed = s_ref[:, 24:32, :]
    c_ref[0] = packed.reshape(256, 128) * (1.0 / 18.0)
    rest = jnp.broadcast_to(halo[:, 3:4, :], shape).reshape(256, 128)
    rest = jnp.stack([pltpu.roll(rest[8 * i : 8 * i + 8], 112, 1, stride=2, stride_axis=0) for i in range(32)])
    depth = jnp.where(slot >= 4, jnp.where(col < 5, roll(packed, 53, 2), roll(packed, 26, 2)), jnp.where(col < 7, roll(packed, -73, 2), rest))
    c_ref[1] = depth.reshape(256, 128) * (1.0 / 18.0)
    for i in range(32):
        whole = jnp.concatenate([s_ref[i, 0:24, :], h_ref[i]], axis=0)
        v, at = divmod(24 * i, 128)
        here = min(24, 128 - at)
        for n, p in enumerate(planes):
            moved = roll(whole, at - 24 * p, 1)
            f_ref[n, :, 128 * v + at : 128 * v + at + here] = moved[:, at : at + here]
            if here < 24:
                f_ref[n, :, 128 * v + 128 : 128 * v + 128 + 24 - here] = moved[:, : 24 - here]


def refine(coarse, y_ref, hats_ref, p_ref, out_ref):
    both = two_pieces(coarse.T)
    for n in range(3):
        part = slice(256 * n, 256 * n + 256)
        fine = jnp.dot(both, y_ref[:, part], preferred_element_type=F32)
        p_ref[:, part] = two_pieces(fine[:128] + fine[128:])
    for n in range(3):
        part = slice(256 * n, 256 * n + 256)
        out_ref[:, part] = jnp.dot(hats_ref[...], p_ref[:, part], preferred_element_type=F32)


def plane_sweeps(f_ref, u_ref, x_ref, q_ref, b_ref, count):
    def along_x(v, carry):
        part = pl.ds(pl.multiple_of(128 * v, 128), 128)
        for p in range(count):
            u = u_ref[32 * p : 32 * p + 32, part]
            terms = remesh_terms(u, roll(u, 1, 0), roll(u, -1, 0), f_ref[p, :, part])
            for n, m in enumerate((1, -1, 2, -2, 3, -3)):
                if m > 0:
                    b_ref[p, n, 0:8, :] = terms[m][24:32]
                    b_ref[p, n, 8:32, :] = terms[m][0:24]
                else:
                    b_ref[p, n, 8:40, :] = terms[m]
            total = terms[0][:24]
            for n, m in enumerate((1, -1, 2, -2, 3, -3)):
                total = total + b_ref[p, n, 8 - m : 32 - m, :]
            x_ref[p, :, part] = total
        return carry

    lax.fori_loop(0, 6, along_x, 0)

    def along_y(t, carry):
        for p in range(count):
            rows = pl.ds(pl.multiple_of(8 * t, 8), 8)
            speed = u_ref[pl.ds(pl.multiple_of(32 * count + 24 * p + 8 * t, 8), 8), :]
            q_ref[p, rows, :] = sweep_ring(x_ref[p, rows, :], speed, 1)
        return carry

    lax.fori_loop(0, 3, along_y, 0)


def near_planes(s_ref, y_ref, hats_ref, hats_z_ref, outer_ref, q_ref, f_ref, c_ref, h_ref, p_ref, u_ref, w_ref, x_ref, b_ref):
    unpack(s_ref, f_ref, c_ref, h_ref, (0, 1, 2))
    refine(c_ref[0], y_ref, hats_ref, p_ref, u_ref)
    refine(c_ref[1], y_ref, hats_z_ref, p_ref, w_ref)
    plane_sweeps(f_ref, u_ref, x_ref, q_ref, b_ref, 3)

    def along_z(v, carry):
        part = pl.ds(pl.multiple_of(128 * v, 128), 128)
        for t in range(3):
            rows = slice(8 * t, 8 * t + 8)
            speeds = [w_ref[24 * p + 8 * t : 24 * p + 8 * t + 8, part] for p in range(5)]
            first, second, third = [remesh_terms(speeds[p + 1], speeds[p], speeds[p + 2], q_ref[p, rows, part]) for p in range(3)]
            outer_ref[0, rows, part] = first[-1] + second[-2] + third[-3]
            outer_ref[1, rows, part] = first[-2] + second[-3]
            outer_ref[2, rows, part] = first[-3]
        return carry

    lax.fori_loop(0, 6, along_z, 0)


def far_plane(s_ref, y_ref, hats_ref, hats_z_ref, near_ref, own_ref, inner_ref, f_ref, c_ref, h_ref, p_ref, u_ref, w_ref, x_ref, b_ref, q_ref):
    unpack(s_ref, f_ref, c_ref, h_ref, (3,))
    refine(c_ref[0], y_ref, hats_ref, p_ref, u_ref)
    refine(c_ref[1], y_ref, hats_z_ref, p_ref, w_ref)
    plane_sweeps(f_ref, u_ref, x_ref, q_ref, b_ref, 1)

    def along_z(v, carry):
        part = pl.ds(pl.multiple_of(128 * v, 128), 128)
        for t in range(3):
            rows = slice(8 * t, 8 * t + 8)
            speeds = [w_ref[24 * p + 8 * t : 24 * p + 8 * t + 8, part] for p in range(6)]
            total = {}
            for p in range(4):
                q = q_ref[0, rows, part] if p == 3 else near_ref[p, rows, part]
                terms = remesh_terms(speeds[p + 1], speeds[p], speeds[p + 2], q)
                for m, term in terms.items():
                    total[p + m] = total[p + m] + term if p + m in total else term
            for n in range(4):
                own_ref[n, rows, part] = total[n]
            for n in range(3):
                inner_ref[n, rows, part] = total[4 + n]
        return carry

    lax.fori_loop(0, 6, along_z, 0)


def join(own_ref, outer_ref, inner_ref, out_ref):
    flip = odd_device() * 3
    scale = 1.0 / 27.0
    out_ref[0 ^ flip] = (own_ref[0] + outer_ref[0]) * scale
    out_ref[1 ^ flip] = (own_ref[1] + outer_ref[1] + inner_ref[2]) * scale
    out_ref[2 ^ flip] = (own_ref[2] + outer_ref[2] + inner_ref[1]) * scale
    out_ref[3 ^ flip] = (own_ref[3] + inner_ref[0]) * scale


def kernel(body, *shapes, scratch=(), flops=1e7, specs=None):
    outs = tuple(jax.ShapeDtypeStruct(*(s if isinstance(s[0], tuple) else (s, F32))) for s in shapes)
    extra = {"in_specs": [pl.BlockSpec(memory_space=m) for m in specs]} if specs else {}
    return pl.pallas_call(
        body,
        out_shape=outs if len(outs) > 1 else outs[0],
        scratch_shapes=[pltpu.VMEM(*(s if isinstance(s[0], tuple) else (s, F32))) for s in scratch],
        cost_estimate=pl.CostEstimate(flops=int(flops), transcendentals=0, bytes_accessed=1 << 20),
        compiler_params=pltpu.CompilerParams(vmem_limit_bytes=16 * 1024 * 1024),
        **extra,
    )


def exchange(x, axis):
    return lax.all_to_all(x, axis, split_axis=0, concat_axis=0, tiled=False)


def sweep_scratch(count, speeds):
    return [(count, 32, 768), (2, 256, 128), (32, 8, 128), ((256, 768), BF16), (56 * count, 768), (24 * speeds, 768), (count, 24, 768), (count, 6, 40, 128)]


def steps(scalar, velocity):
    tables = [(t, BF16) for t in ((256, 768), (168, 256), (120, 256), (56, 256), (144, 256))]
    y_weights, near, near_z, far, far_z = kernel(weights, *tables, flops=1e9)()
    coarse = jnp.transpose(velocity, (0, 2, 3, 1))
    planes = exchange(kernel(pack_velocity, (16, 16, 128), specs=(pltpu.VMEM, pl.ANY))(coarse, near), "gz")
    chunks = exchange(kernel(pack_chunks, (32, 32, 128), scratch=[(768, 128)])(scalar, planes), "gy")
    outer, swept = kernel(near_planes, (3, 24, 768), (3, 24, 768), scratch=sweep_scratch(3, 5))(chunks, y_weights, near, near_z)
    count = lax.axis_size("gz")
    pairs = [(k, k + 1) for k in range(1, count - 1, 2)]
    outer = lax.ppermute(outer, "gz", pairs + [(b, a) for a, b in pairs])
    own, inner = kernel(far_plane, (4, 24, 768), (3, 24, 768), scratch=sweep_scratch(1, 6) + [(1, 24, 768)], flops=1e9)(chunks, y_weights, far, far_z, swept)
    pairs = [(k, k + 1) for k in range(0, count, 2)]
    inner = lax.ppermute(inner, "gz", pairs + [(b, a) for a, b in pairs])
    return kernel(join, (4, 24, 768))(own, outer, inner)


def solution(mesh):
    in_specs = (P("gz", "gy", None), P(None, None, "gy", "gz"))
    out_specs = P("gz", "gy", None)
    return jax.shard_map(steps, mesh=mesh, in_specs=in_specs, out_specs=out_specs, check_vma=False)
```

```python
import jax
import jax.numpy as jnp
from jax import lax
from jax.experimental import pallas as pl
from jax.experimental.pallas import tpu as pltpu
from jax.sharding import PartitionSpec as P


F32 = jnp.float32
BF16 = jnp.bfloat16


def iota(shape, dim):
    return lax.broadcasted_iota(jnp.int32, shape, dim)


def remesh_terms(h, before, after, q):
    up = h >= 0.0
    b = jnp.abs(h - jnp.abs(h) * (h - jnp.where(up, after, before))) - 0.25
    s = b * b
    g1, g3, g5 = s - 1.0 / 16.0, s - 9.0 / 16.0, s - 25.0 / 16.0
    e2 = g1 * g3
    e1 = (g1 * g5) * -3.0
    e0 = (g3 * g5) * 2.0
    g = g1 * b
    o2 = g * (3.25 - 20.0 * s)
    o1 = g * (100.0 * s - 20.25)
    o0 = g * (44.5 - 200.0 * s) - 6.0 * b
    at0 = q * (e0 + o0)
    near1, far1 = q * (e0 - o0), q * (e1 + o1)
    near2, far2 = q * (e1 - o1), q * (e2 + o2)
    near3 = q * (e2 - o2)
    zero = jnp.zeros_like(q)
    return {
        0: at0,
        1: jnp.where(up, near1, far1),
        -1: jnp.where(up, far1, near1),
        2: jnp.where(up, near2, far2),
        -2: jnp.where(up, far2, near2),
        3: jnp.where(up, near3, zero),
        -3: jnp.where(up, zero, near3),
    }


def roll(x, shift, axis):
    n = x.shape[axis]
    shift = shift % n
    return x if shift == 0 else pltpu.roll(x, shift, axis)


def sweep_ring(q, u, axis):
    terms = remesh_terms(u, roll(u, 1, axis), roll(u, -1, axis), q)
    total = terms[0]
    for m in (1, -1, 2, -2, 3, -3):
        total = total + roll(terms[m], m, axis)
    return total


def swap_blocks(x):
    row = iota((8, 128), 0)
    block = iota((8, 128), 1) >> 4
    for bit in (1, 2, 4):
        low = (row & bit) == 0
        first = (block & bit) == 0
        upward = roll(roll(x, -bit, 0), 16 * bit, 1)
        downward = roll(roll(x, bit, 0), -16 * bit, 1)
        x = jnp.where(low == first, x, jnp.where(low, upward, downward))
    return x


def pack_velocity(v_ref, after_ref, out_ref):
    lane = iota((8, 128), 1)
    tiles = []
    for c in range(3):
        block = v_ref[c].reshape(128, 64)
        block = jnp.concatenate([block, jnp.zeros((128, 64), F32)], axis=1).T
        tiles.append([swap_blocks(block[8 * n : 8 * n + 8]) for n in range(8)])
    zero = jnp.zeros((8, 128), F32)
    for k in range(16):
        n, odd = divmod(k, 2)
        if odd == 0:
            out_ref[k, 0:8, :] = jnp.where(lane < 64, tiles[0][n], roll(tiles[1][n], 64, 1))
            before = tiles[2][n - 1] if n > 0 else zero
            planes = jnp.where(lane < 16, roll(before, 16, 1), roll(tiles[2][n], 16, 1))
        else:
            out_ref[k, 0:8, :] = jnp.where(lane < 64, roll(tiles[0][n], -64, 1), tiles[1][n])
            after = tiles[2][n + 1] if n < 7 else zero
            planes = jnp.where(lane < 80, roll(tiles[2][n], -48, 1), roll(after, 80, 1))
        out_ref[k, 8:16, :] = jnp.where(lane < 96, planes, zero)


def odd_device():
    return lax.axis_index("gz") & 1


def pack_chunks(s_ref, r_ref, out_ref, t_ref):
    flip = odd_device() * 3
    for v in range(6):
        part = slice(128 * v, 128 * v + 128)
        block = jnp.concatenate([s_ref[p ^ flip, :, part] for p in range(4)] + [jnp.zeros((32, 128), F32)], axis=0)
        t_ref[part, :] = block.T
    shape = (16, 8, 128)
    lane = iota(shape, 2)
    row = iota(shape, 1)
    col = lane & 15
    slot = lane >> 4

    def block(x, step):
        return jnp.concatenate([x[step:], x[:step]], axis=0)

    here, depth = r_ref[:, 0:8, :], r_ref[:, 8:16, :]
    wide = jnp.where(col == 0, block(roll(here, -15, 2), -1), roll(here, 1, 2))
    even = (wide, here, depth)
    wide = jnp.where(col < 9, roll(here, -7, 2), block(roll(here, 9, 2), 1))
    near = jnp.where(col < 8, roll(here, -8, 2), block(roll(here, 8, 2), 1))
    depth = jnp.where(col < 8, roll(depth, -8, 2), block(roll(depth, 8, 2), 1))
    stash = []
    for parity, (wide, near, depth) in enumerate((even, (wide, near, depth))):
        tile = jnp.where(slot < 4, wide, near)
        tile = jnp.where((slot >= 4) & (col >= 9), roll(depth, 73, 2), tile)
        tile = jnp.where((slot < 2) & (col >= 11), roll(depth, -53, 2), tile)
        tile = jnp.where(((slot >> 1) == 1) & (col >= 11), roll(depth, -26, 2), tile)
        rest = jnp.where((slot < 4) & ((col == 7) | (col == 8)), depth, 0.0)
        for bit in (1, 2, 4):
            rest = jnp.where((row & bit) == 0, roll(rest, -bit, 1), roll(rest, bit, 1))
        rest = jnp.stack([pltpu.roll(rest[n], 0, 1, stride=2, stride_axis=0) for n in range(16)])
        for bit in (4, 2, 1):
            rest = rest + roll(rest, bit, 1)
        stash.append(rest)
        for n in range(16):
            out_ref[2 * n + parity, 24:32, :] = tile[n]
    lane = iota((8, 128), 1)
    row = iota((8, 128), 0)
    for i in range(32):
        left = t_ref[(24 * i - 8) % 768 : (24 * i - 8) % 768 + 8, :]
        right = t_ref[(24 * i + 24) % 768 : (24 * i + 24) % 768 + 8, :]
        halo = jnp.where(row < 3, right, jnp.where(row == 3, stash[i % 2][i // 2], left))
        for t in range(3):
            tile = t_ref[24 * i + 8 * t : 24 * i + 8 * t + 8, :]
            out_ref[i, 8 * t : 8 * t + 8, :] = jnp.where(lane < 96, tile, roll(halo, 96 - 32 * t, 1))


def hat_rows(rows, slot, ring):
    e = iota((rows, 128), 0)
    if ring:
        e = jnp.where(e > 28, e - 32, e) + 3
    lane = iota((rows, 128), 1)
    away = jnp.abs(e - 3 * (lane & 15))
    return jnp.where((lane >> 4) == slot, jnp.maximum(3 - away, 0), 0)


def weights(y_ref, near_ref, near_z_ref, far_ref, far_z_ref):
    odd = odd_device()
    for v in range(6):
        c = iota((256, 128), 0)
        f = iota((256, 128), 1) + 128 * v
        away = jnp.abs(f - 3 * c)
        away = jnp.minimum(away, 768 - away)
        y_ref[:, 128 * v : 128 * v + 128] = jnp.maximum(3 - away, 0).astype(F32).astype(BF16)

    def both(rows):
        return jnp.concatenate(rows, axis=0).astype(F32).astype(BF16)

    sign = 1 - 2 * odd
    for planes, speeds, xy_ref, z_ref in (((0, 1, 2), range(5), near_ref, near_z_ref), ((3,), range(6), far_ref, far_z_ref)):
        xy = both([hat_rows(32, p ^ (3 * odd), True) for p in planes] + [hat_rows(24, 4 + (p ^ (3 * odd)), False) for p in planes])
        z = both([hat_rows(24, jnp.where(odd == 1, 5 - p, p), False) * sign for p in speeds])
        xy_ref[:, 0:128] = xy
        xy_ref[:, 128:256] = xy
        z_ref[:, 0:128] = z
        z_ref[:, 128:256] = z


def two_pieces(x):
    hi = x.astype(BF16)
    return jnp.concatenate([hi, (x - hi.astype(F32)).astype(BF16)], axis=0)


def unpack(s_ref, f_ref, c_ref, h_ref, planes):
    shape = (32, 8, 128)
    lane = iota(shape, 2)
    row = iota(shape, 1)
    col = lane & 15
    slot = lane >> 4
    parts = [roll(s_ref[:, 8 * t : 8 * t + 8, :], 32 * t - 96, 2) for t in range(3)]
    halo = jnp.where(lane < 32, parts[0], jnp.where(lane < 64, parts[1], parts[2]))
    h_ref[...] = halo
    packed = s_ref[:, 24:32, :]
    c_ref[0] = packed.reshape(256, 128) * (1.0 / 18.0)
    rest = jnp.broadcast_to(halo[:, 3:4, :], shape).reshape(256, 128)
    rest = jnp.stack([pltpu.roll(rest[8 * i : 8 * i + 8], 114, 1, stride=2, stride_axis=0) for i in range(32)])
    depth = jnp.where(slot >= 4, jnp.where(col < 5, roll(packed, 53, 2), roll(packed, 26, 2)), jnp.where(col < 7, roll(packed, -73, 2), rest))
    c_ref[1] = depth.reshape(256, 128) * (1.0 / 18.0)
    for i in range(32):
        whole = jnp.concatenate([s_ref[i, 0:24, :], h_ref[i]], axis=0)
        v, at = divmod(24 * i, 128)
        here = min(24, 128 - at)
        for n, p in enumerate(planes):
            moved = roll(whole, at - 24 * p, 1)
            f_ref[n, :, 128 * v + at : 128 * v + at + here] = moved[:, at : at + here]
            if here < 24:
                f_ref[n, :, 128 * v + 128 : 128 * v + 128 + 24 - here] = moved[:, : 24 - here]


def refine(coarse, y_ref, hats_ref, p_ref, out_ref):
    both = two_pieces(coarse.T)
    for n in range(3):
        part = slice(256 * n, 256 * n + 256)
        fine = jnp.dot(both, y_ref[:, part], preferred_element_type=F32)
        p_ref[:, part] = two_pieces(fine[:128] + fine[128:])
    for n in range(3):
        part = slice(256 * n, 256 * n + 256)
        out_ref[:, part] = jnp.dot(hats_ref[...], p_ref[:, part], preferred_element_type=F32)


def plane_sweeps(f_ref, u_ref, x_ref, q_ref, b_ref, count):
    def along_x(v, carry):
        part = pl.ds(pl.multiple_of(128 * v, 128), 128)
        for p in range(count):
            u = u_ref[32 * p : 32 * p + 32, part]
            terms = remesh_terms(u, roll(u, 1, 0), roll(u, -1, 0), f_ref[p, :, part])
            for n, m in enumerate((1, -1, 2, -2, 3, -3)):
                if m > 0:
                    b_ref[p, n, 0:8, :] = terms[m][24:32]
                    b_ref[p, n, 8:32, :] = terms[m][0:24]
                else:
                    b_ref[p, n, 8:40, :] = terms[m]
            total = terms[0][:24]
            for n, m in enumerate((1, -1, 2, -2, 3, -3)):
                total = total + b_ref[p, n, 8 - m : 32 - m, :]
            x_ref[p, :, part] = total
        return carry

    lax.fori_loop(0, 6, along_x, 0)

    def along_y(t, carry):
        for p in range(count):
            rows = pl.ds(pl.multiple_of(8 * t, 8), 8)
            speed = u_ref[pl.ds(pl.multiple_of(32 * count + 24 * p + 8 * t, 8), 8), :]
            q_ref[p, rows, :] = sweep_ring(x_ref[p, rows, :], speed, 1)
        return carry

    lax.fori_loop(0, 3, along_y, 0)


def near_planes(s_ref, y_ref, hats_ref, hats_z_ref, outer_ref, q_ref, f_ref, c_ref, h_ref, p_ref, u_ref, w_ref, x_ref, b_ref):
    unpack(s_ref, f_ref, c_ref, h_ref, (0, 1, 2))
    refine(c_ref[0], y_ref, hats_ref, p_ref, u_ref)
    refine(c_ref[1], y_ref, hats_z_ref, p_ref, w_ref)
    plane_sweeps(f_ref, u_ref, x_ref, q_ref, b_ref, 3)

    def along_z(v, carry):
        part = pl.ds(pl.multiple_of(128 * v, 128), 128)
        for t in range(3):
            rows = slice(8 * t, 8 * t + 8)
            speeds = [w_ref[24 * p + 8 * t : 24 * p + 8 * t + 8, part] for p in range(5)]
            first, second, third = [remesh_terms(speeds[p + 1], speeds[p], speeds[p + 2], q_ref[p, rows, part]) for p in range(3)]
            outer_ref[0, rows, part] = first[-1] + second[-2] + third[-3]
            outer_ref[1, rows, part] = first[-2] + second[-3]
            outer_ref[2, rows, part] = first[-3]
        return carry

    lax.fori_loop(0, 6, along_z, 0)


def far_plane(s_ref, y_ref, hats_ref, hats_z_ref, near_ref, own_ref, inner_ref, f_ref, c_ref, h_ref, p_ref, u_ref, w_ref, x_ref, b_ref, q_ref):
    unpack(s_ref, f_ref, c_ref, h_ref, (3,))
    refine(c_ref[0], y_ref, hats_ref, p_ref, u_ref)
    refine(c_ref[1], y_ref, hats_z_ref, p_ref, w_ref)
    plane_sweeps(f_ref, u_ref, x_ref, q_ref, b_ref, 1)

    def along_z(v, carry):
        part = pl.ds(pl.multiple_of(128 * v, 128), 128)
        for t in range(3):
            rows = slice(8 * t, 8 * t + 8)
            speeds = [w_ref[24 * p + 8 * t : 24 * p + 8 * t + 8, part] for p in range(6)]
            total = {}
            for p in range(4):
                q = q_ref[0, rows, part] if p == 3 else near_ref[p, rows, part]
                terms = remesh_terms(speeds[p + 1], speeds[p], speeds[p + 2], q)
                for m, term in terms.items():
                    total[p + m] = total[p + m] + term if p + m in total else term
            for n in range(4):
                own_ref[n, rows, part] = total[n]
            for n in range(3):
                inner_ref[n, rows, part] = total[4 + n]
        return carry

    lax.fori_loop(0, 6, along_z, 0)


def join(own_ref, outer_ref, inner_ref, out_ref):
    flip = odd_device() * 3
    scale = 1.0 / 27.0
    out_ref[0 ^ flip] = (own_ref[0] + outer_ref[0]) * scale
    out_ref[1 ^ flip] = (own_ref[1] + outer_ref[1] + inner_ref[2]) * scale
    out_ref[2 ^ flip] = (own_ref[2] + outer_ref[2] + inner_ref[1]) * scale
    out_ref[3 ^ flip] = (own_ref[3] + inner_ref[0]) * scale


def kernel(body, *shapes, scratch=(), flops=1e7, specs=None):
    outs = tuple(jax.ShapeDtypeStruct(*(s if isinstance(s[0], tuple) else (s, F32))) for s in shapes)
    extra = {"in_specs": [pl.BlockSpec(memory_space=m) for m in specs]} if specs else {}
    return pl.pallas_call(
        body,
        out_shape=outs if len(outs) > 1 else outs[0],
        scratch_shapes=[pltpu.VMEM(*(s if isinstance(s[0], tuple) else (s, F32))) for s in scratch],
        cost_estimate=pl.CostEstimate(flops=int(flops), transcendentals=0, bytes_accessed=1 << 20),
        compiler_params=pltpu.CompilerParams(vmem_limit_bytes=16 * 1024 * 1024),
        **extra,
    )


def exchange(x, axis):
    return lax.all_to_all(x, axis, split_axis=0, concat_axis=0, tiled=False)


def sweep_scratch(count, speeds):
    return [(count, 32, 768), (2, 256, 128), (32, 8, 128), ((256, 768), BF16), (56 * count, 768), (24 * speeds, 768), (count, 24, 768), (count, 6, 40, 128)]


def steps(scalar, velocity):
    tables = [(t, BF16) for t in ((256, 768), (168, 256), (120, 256), (56, 256), (144, 256))]
    y_weights, near, near_z, far, far_z = kernel(weights, *tables, flops=1e9)()
    coarse = jnp.transpose(velocity, (0, 2, 3, 1))
    planes = exchange(kernel(pack_velocity, (16, 16, 128), specs=(pltpu.VMEM, pl.ANY))(coarse, near), "gz")
    chunks = exchange(kernel(pack_chunks, (32, 32, 128), scratch=[(768, 128)])(scalar, planes), "gy")
    outer, swept = kernel(near_planes, (3, 24, 768), (3, 24, 768), scratch=sweep_scratch(3, 5))(chunks, y_weights, near, near_z)
    count = lax.axis_size("gz")
    pairs = [(k, k + 1) for k in range(1, count - 1, 2)]
    outer = lax.ppermute(outer, "gz", pairs + [(b, a) for a, b in pairs])
    own, inner = kernel(far_plane, (4, 24, 768), (3, 24, 768), scratch=sweep_scratch(1, 6) + [(1, 24, 768)], flops=1e9)(chunks, y_weights, far, far_z, swept)
    pairs = [(k, k + 1) for k in range(0, count, 2)]
    inner = lax.ppermute(inner, "gz", pairs + [(b, a) for a, b in pairs])
    return kernel(join, (4, 24, 768))(own, outer, inner)


def solution(mesh):
    in_specs = (P("gz", "gy", None), P(None, None, "gy", "gz"))
    out_specs = P("gz", "gy", None)
    return jax.shard_map(steps, mesh=mesh, in_specs=in_specs, out_specs=out_specs, check_vma=False)
```

```python
import jax
import jax.numpy as jnp
from jax import lax
from jax.experimental import pallas as pl
from jax.experimental.pallas import tpu as pltpu
from jax.sharding import PartitionSpec as P


F32 = jnp.float32
BF16 = jnp.bfloat16


def iota(shape, dim):
    return lax.broadcasted_iota(jnp.int32, shape, dim)


def remesh_terms(h, before, after, q):
    up = h >= 0.0
    b = jnp.abs(h - jnp.abs(h) * (h - jnp.where(up, after, before))) - 0.25
    s = b * b
    g1, g3, g5 = s - 1.0 / 16.0, s - 9.0 / 16.0, s - 25.0 / 16.0
    e2 = g1 * g3
    e1 = (g1 * g5) * -3.0
    e0 = (g3 * g5) * 2.0
    g = g1 * b
    o2 = g * (3.25 - 20.0 * s)
    o1 = g * (100.0 * s - 20.25)
    o0 = g * (44.5 - 200.0 * s) - 6.0 * b
    at0 = q * (e0 + o0)
    near1, far1 = q * (e0 - o0), q * (e1 + o1)
    near2, far2 = q * (e1 - o1), q * (e2 + o2)
    near3 = q * (e2 - o2)
    zero = jnp.zeros_like(q)
    return {
        0: at0,
        1: jnp.where(up, near1, far1),
        -1: jnp.where(up, far1, near1),
        2: jnp.where(up, near2, far2),
        -2: jnp.where(up, far2, near2),
        3: jnp.where(up, near3, zero),
        -3: jnp.where(up, zero, near3),
    }


def roll(x, shift, axis):
    n = x.shape[axis]
    shift = shift % n
    return x if shift == 0 else pltpu.roll(x, shift, axis)


def sweep_ring(q, u, axis):
    terms = remesh_terms(u, roll(u, 1, axis), roll(u, -1, axis), q)
    total = terms[0]
    for m in (1, -1, 2, -2, 3, -3):
        total = total + roll(terms[m], m, axis)
    return total


def swap_blocks(x):
    row = iota((8, 128), 0)
    block = iota((8, 128), 1) >> 4
    for bit in (1, 2, 4):
        low = (row & bit) == 0
        first = (block & bit) == 0
        upward = roll(roll(x, -bit, 0), 16 * bit, 1)
        downward = roll(roll(x, bit, 0), -16 * bit, 1)
        x = jnp.where(low == first, x, jnp.where(low, upward, downward))
    return x


def pack_velocity(v_ref, after_ref, out_ref):
    lane = iota((8, 128), 1)
    tiles = []
    for c in range(3):
        block = v_ref[c].reshape(128, 64)
        block = jnp.concatenate([block, jnp.zeros((128, 64), F32)], axis=1).T
        tiles.append([swap_blocks(block[8 * n : 8 * n + 8]) for n in range(8)])
    zero = jnp.zeros((8, 128), F32)
    for k in range(16):
        n, odd = divmod(k, 2)
        if odd == 0:
            out_ref[k, 0:8, :] = jnp.where(lane < 64, tiles[0][n], roll(tiles[1][n], 64, 1))
            before = tiles[2][n - 1] if n > 0 else zero
            planes = jnp.where(lane < 16, roll(before, 16, 1), roll(tiles[2][n], 16, 1))
        else:
            out_ref[k, 0:8, :] = jnp.where(lane < 64, roll(tiles[0][n], -64, 1), tiles[1][n])
            after = tiles[2][n + 1] if n < 7 else zero
            planes = jnp.where(lane < 80, roll(tiles[2][n], -48, 1), roll(after, 80, 1))
        out_ref[k, 8:16, :] = jnp.where(lane < 96, planes, zero)


def odd_device():
    return lax.axis_index("gz") & 1


def pack_chunks(s_ref, r_ref, out_ref, t_ref):
    shape = (16, 8, 128)
    lane = iota(shape, 2)
    row = iota(shape, 1)
    col = lane & 15
    slot = lane >> 4

    def block(x, step):
        return jnp.concatenate([x[step:], x[:step]], axis=0)

    here, depth = r_ref[:, 0:8, :], r_ref[:, 8:16, :]
    wide = jnp.where(col == 0, block(roll(here, -15, 2), -1), roll(here, 1, 2))
    even = (wide, here, depth)
    wide = jnp.where(col < 9, roll(here, -7, 2), block(roll(here, 9, 2), 1))
    near = jnp.where(col < 8, roll(here, -8, 2), block(roll(here, 8, 2), 1))
    depth = jnp.where(col < 8, roll(depth, -8, 2), block(roll(depth, 8, 2), 1))
    stash = []
    for parity, (wide, near, depth) in enumerate((even, (wide, near, depth))):
        tile = jnp.where(slot < 4, wide, near)
        tile = jnp.where((slot >= 4) & (col >= 9), roll(depth, 73, 2), tile)
        tile = jnp.where((slot < 2) & (col >= 11), roll(depth, -53, 2), tile)
        tile = jnp.where(((slot >> 1) == 1) & (col >= 11), roll(depth, -26, 2), tile)
        rest = jnp.where((slot < 4) & ((col == 7) | (col == 8)), depth, 0.0)
        for bit in (1, 2, 4):
            rest = jnp.where((row & bit) == 0, roll(rest, -bit, 1), roll(rest, bit, 1))
        rest = jnp.stack([pltpu.roll(rest[n], 0, 1, stride=2, stride_axis=0) for n in range(16)])
        for bit in (4, 2, 1):
            rest = rest + roll(rest, bit, 1)
        stash.append(rest)
        for n in range(16):
            out_ref[2 * n + parity, 24:32, :] = tile[n]
    flip = odd_device() * 3
    for v in range(6):
        part = slice(128 * v, 128 * v + 128)
        block = jnp.concatenate([s_ref[p ^ flip, :, part] for p in range(4)] + [jnp.zeros((32, 128), F32)], axis=0)
        t_ref[part, :] = block.T
    lane = iota((8, 128), 1)
    row = iota((8, 128), 0)
    for i in range(32):
        left = t_ref[(24 * i - 8) % 768 : (24 * i - 8) % 768 + 8, :]
        right = t_ref[(24 * i + 24) % 768 : (24 * i + 24) % 768 + 8, :]
        halo = jnp.where(row < 3, right, jnp.where(row == 3, stash[i % 2][i // 2], left))
        for t in range(3):
            tile = t_ref[24 * i + 8 * t : 24 * i + 8 * t + 8, :]
            out_ref[i, 8 * t : 8 * t + 8, :] = jnp.where(lane < 96, tile, roll(halo, 96 - 32 * t, 1))


def hat_rows(rows, slot, ring):
    e = iota((rows, 128), 0)
    if ring:
        e = jnp.where(e > 28, e - 32, e) + 3
    lane = iota((rows, 128), 1)
    away = jnp.abs(e - 3 * (lane & 15))
    return jnp.where((lane >> 4) == slot, jnp.maximum(3 - away, 0), 0)


def weights(y_ref, near_ref, near_z_ref, far_ref, far_z_ref):
    odd = odd_device()
    for v in range(6):
        c = iota((256, 128), 0)
        f = iota((256, 128), 1) + 128 * v
        away = jnp.abs(f - 3 * c)
        away = jnp.minimum(away, 768 - away)
        y_ref[:, 128 * v : 128 * v + 128] = jnp.maximum(3 - away, 0).astype(F32).astype(BF16)

    def both(rows):
        return jnp.concatenate(rows, axis=0).astype(F32).astype(BF16)

    sign = 1 - 2 * odd
    for planes, speeds, xy_ref, z_ref in (((0, 1, 2), range(5), near_ref, near_z_ref), ((3,), range(6), far_ref, far_z_ref)):
        xy = both([hat_rows(32, p ^ (3 * odd), True) for p in planes] + [hat_rows(24, 4 + (p ^ (3 * odd)), False) for p in planes])
        z = both([hat_rows(24, jnp.where(odd == 1, 5 - p, p), False) * sign for p in speeds])
        xy_ref[:, 0:128] = xy
        xy_ref[:, 128:256] = xy
        z_ref[:, 0:128] = z
        z_ref[:, 128:256] = z


def two_pieces(x):
    hi = x.astype(BF16)
    return jnp.concatenate([hi, (x - hi.astype(F32)).astype(BF16)], axis=0)


def unpack(s_ref, f_ref, c_ref, h_ref, planes):
    shape = (32, 8, 128)
    lane = iota(shape, 2)
    row = iota(shape, 1)
    col = lane & 15
    slot = lane >> 4
    parts = [roll(s_ref[:, 8 * t : 8 * t + 8, :], 32 * t - 96, 2) for t in range(3)]
    halo = jnp.where(lane < 32, parts[0], jnp.where(lane < 64, parts[1], parts[2]))
    h_ref[...] = halo
    packed = s_ref[:, 24:32, :]
    c_ref[0] = packed.reshape(256, 128) * (1.0 / 18.0)
    rest = jnp.broadcast_to(halo[:, 3:4, :], shape).reshape(256, 128)
    rest = jnp.stack([pltpu.roll(rest[8 * i : 8 * i + 8], 114, 1, stride=2, stride_axis=0) for i in range(32)])
    depth = jnp.where(slot >= 4, jnp.where(col < 5, roll(packed, 53, 2), roll(packed, 26, 2)), jnp.where(col < 7, roll(packed, -73, 2), rest))
    c_ref[1] = depth.reshape(256, 128) * (1.0 / 18.0)
    for i in range(32):
        whole = jnp.concatenate([s_ref[i, 0:24, :], h_ref[i]], axis=0)
        v, at = divmod(24 * i, 128)
        here = min(24, 128 - at)
        for n, p in enumerate(planes):
            moved = roll(whole, at - 24 * p, 1)
            f_ref[n, :, 128 * v + at : 128 * v + at + here] = moved[:, at : at + here]
            if here < 24:
                f_ref[n, :, 128 * v + 128 : 128 * v + 128 + 24 - here] = moved[:, : 24 - here]


def refine(coarse, y_ref, hats_ref, p_ref, out_ref):
    both = two_pieces(coarse.T)
    for n in range(3):
        part = slice(256 * n, 256 * n + 256)
        fine = jnp.dot(both, y_ref[:, part], preferred_element_type=F32)
        p_ref[:, part] = two_pieces(fine[:128] + fine[128:])
    for n in range(3):
        part = slice(256 * n, 256 * n + 256)
        out_ref[:, part] = jnp.dot(hats_ref[...], p_ref[:, part], preferred_element_type=F32)


def plane_sweeps(f_ref, u_ref, x_ref, q_ref, b_ref, count):
    def along_x(v, carry):
        part = pl.ds(pl.multiple_of(128 * v, 128), 128)
        for p in range(count):
            u = u_ref[32 * p : 32 * p + 32, part]
            terms = remesh_terms(u, roll(u, 1, 0), roll(u, -1, 0), f_ref[p, :, part])
            for n, m in enumerate((1, -1, 2, -2, 3, -3)):
                if m > 0:
                    b_ref[p, n, 0:8, :] = terms[m][24:32]
                    b_ref[p, n, 8:32, :] = terms[m][0:24]
                else:
                    b_ref[p, n, 8:40, :] = terms[m]
            total = terms[0][:24]
            for n, m in enumerate((1, -1, 2, -2, 3, -3)):
                total = total + b_ref[p, n, 8 - m : 32 - m, :]
            x_ref[p, :, part] = total
        return carry

    lax.fori_loop(0, 6, along_x, 0, unroll=True)

    def along_y(t, carry):
        for p in range(count):
            rows = pl.ds(pl.multiple_of(8 * t, 8), 8)
            speed = u_ref[pl.ds(pl.multiple_of(32 * count + 24 * p + 8 * t, 8), 8), :]
            q_ref[p, rows, :] = sweep_ring(x_ref[p, rows, :], speed, 1)
        return carry

    lax.fori_loop(0, 3, along_y, 0)


def near_planes(s_ref, y_ref, hats_ref, hats_z_ref, outer_ref, q_ref, f_ref, c_ref, h_ref, p_ref, u_ref, w_ref, x_ref, b_ref):
    unpack(s_ref, f_ref, c_ref, h_ref, (0, 1, 2))
    refine(c_ref[0], y_ref, hats_ref, p_ref, u_ref)
    refine(c_ref[1], y_ref, hats_z_ref, p_ref, w_ref)
    plane_sweeps(f_ref, u_ref, x_ref, q_ref, b_ref, 3)

    def along_z(v, carry):
        part = pl.ds(pl.multiple_of(128 * v, 128), 128)
        for t in range(3):
            rows = slice(8 * t, 8 * t + 8)
            speeds = [w_ref[24 * p + 8 * t : 24 * p + 8 * t + 8, part] for p in range(5)]
            first, second, third = [remesh_terms(speeds[p + 1], speeds[p], speeds[p + 2], q_ref[p, rows, part]) for p in range(3)]
            outer_ref[0, rows, part] = first[-1] + second[-2] + third[-3]
            outer_ref[1, rows, part] = first[-2] + second[-3]
            outer_ref[2, rows, part] = first[-3]
        return carry

    lax.fori_loop(0, 6, along_z, 0, unroll=True)


def far_plane(s_ref, y_ref, hats_ref, hats_z_ref, near_ref, own_ref, inner_ref, f_ref, c_ref, h_ref, p_ref, u_ref, w_ref, x_ref, b_ref, q_ref):
    unpack(s_ref, f_ref, c_ref, h_ref, (3,))
    refine(c_ref[0], y_ref, hats_ref, p_ref, u_ref)
    refine(c_ref[1], y_ref, hats_z_ref, p_ref, w_ref)
    plane_sweeps(f_ref, u_ref, x_ref, q_ref, b_ref, 1)

    def along_z(v, carry):
        part = pl.ds(pl.multiple_of(128 * v, 128), 128)
        for t in range(3):
            rows = slice(8 * t, 8 * t + 8)
            speeds = [w_ref[24 * p + 8 * t : 24 * p + 8 * t + 8, part] for p in range(6)]
            total = {}
            for p in range(4):
                q = q_ref[0, rows, part] if p == 3 else near_ref[p, rows, part]
                terms = remesh_terms(speeds[p + 1], speeds[p], speeds[p + 2], q)
                for m, term in terms.items():
                    total[p + m] = total[p + m] + term if p + m in total else term
            for n in range(4):
                own_ref[n, rows, part] = total[n]
            for n in range(3):
                inner_ref[n, rows, part] = total[4 + n]
        return carry

    lax.fori_loop(0, 6, along_z, 0, unroll=True)


def join(own_ref, outer_ref, inner_ref, out_ref):
    flip = odd_device() * 3
    scale = 1.0 / 27.0
    out_ref[0 ^ flip] = (own_ref[0] + outer_ref[0]) * scale
    out_ref[1 ^ flip] = (own_ref[1] + outer_ref[1] + inner_ref[2]) * scale
    out_ref[2 ^ flip] = (own_ref[2] + outer_ref[2] + inner_ref[1]) * scale
    out_ref[3 ^ flip] = (own_ref[3] + inner_ref[0]) * scale


def kernel(body, *shapes, scratch=(), flops=1e7, specs=None):
    outs = tuple(jax.ShapeDtypeStruct(*(s if isinstance(s[0], tuple) else (s, F32))) for s in shapes)
    extra = {"in_specs": [pl.BlockSpec(memory_space=m) for m in specs]} if specs else {}
    return pl.pallas_call(
        body,
        out_shape=outs if len(outs) > 1 else outs[0],
        scratch_shapes=[pltpu.VMEM(*(s if isinstance(s[0], tuple) else (s, F32))) for s in scratch],
        cost_estimate=pl.CostEstimate(flops=int(flops), transcendentals=0, bytes_accessed=1 << 20),
        compiler_params=pltpu.CompilerParams(vmem_limit_bytes=16 * 1024 * 1024),
        **extra,
    )


def exchange(x, axis):
    return lax.all_to_all(x, axis, split_axis=0, concat_axis=0, tiled=False)


def sweep_scratch(count, speeds):
    return [(count, 32, 768), (2, 256, 128), (32, 8, 128), ((256, 768), BF16), (56 * count, 768), (24 * speeds, 768), (count, 24, 768), (count, 6, 40, 128)]


def steps(scalar, velocity):
    tables = [(t, BF16) for t in ((256, 768), (168, 256), (120, 256), (56, 256), (144, 256))]
    y_weights, near, near_z, far, far_z = kernel(weights, *tables, flops=1e9)()
    coarse = jnp.transpose(velocity, (0, 2, 3, 1))
    planes = exchange(kernel(pack_velocity, (16, 16, 128), specs=(pltpu.VMEM, pl.ANY))(coarse, near), "gz")
    chunks = exchange(kernel(pack_chunks, (32, 32, 128), scratch=[(768, 128)])(scalar, planes), "gy")
    outer, swept = kernel(near_planes, (3, 24, 768), (3, 24, 768), scratch=sweep_scratch(3, 5))(chunks, y_weights, near, near_z)
    count = lax.axis_size("gz")
    pairs = [(k, k + 1) for k in range(1, count - 1, 2)]
    outer = lax.ppermute(outer, "gz", pairs + [(b, a) for a, b in pairs])
    own, inner = kernel(far_plane, (4, 24, 768), (3, 24, 768), scratch=sweep_scratch(1, 6) + [(1, 24, 768)], flops=1e9)(chunks, y_weights, far, far_z, swept)
    pairs = [(k, k + 1) for k in range(0, count, 2)]
    inner = lax.ppermute(inner, "gz", pairs + [(b, a) for a, b in pairs])
    return kernel(join, (4, 24, 768))(own, outer, inner)


def solution(mesh):
    in_specs = (P("gz", "gy", None), P(None, None, "gy", "gz"))
    out_specs = P("gz", "gy", None)
    return jax.shard_map(steps, mesh=mesh, in_specs=in_specs, out_specs=out_specs, check_vma=False)
```

```python
import jax
import jax.numpy as jnp
from jax import lax
from jax.experimental import pallas as pl
from jax.experimental.pallas import tpu as pltpu
from jax.sharding import PartitionSpec as P


F32 = jnp.float32
BF16 = jnp.bfloat16


def iota(shape, dim):
    return lax.broadcasted_iota(jnp.int32, shape, dim)


def remesh_terms(h, before, after, q):
    up = h >= 0.0
    b = jnp.abs(h - jnp.abs(h) * (h - jnp.where(up, after, before))) - 0.25
    s = b * b
    g1, g3, g5 = s - 1.0 / 16.0, s - 9.0 / 16.0, s - 25.0 / 16.0
    e2 = g1 * g3
    e1 = (g1 * g5) * -3.0
    e0 = (g3 * g5) * 2.0
    g = g1 * b
    o2 = g * (3.25 - 20.0 * s)
    o1 = g * (100.0 * s - 20.25)
    o0 = g * (44.5 - 200.0 * s) - 6.0 * b
    at0 = q * (e0 + o0)
    near1, far1 = q * (e0 - o0), q * (e1 + o1)
    near2, far2 = q * (e1 - o1), q * (e2 + o2)
    near3 = q * (e2 - o2)
    zero = jnp.zeros_like(q)
    return {
        0: at0,
        1: jnp.where(up, near1, far1),
        -1: jnp.where(up, far1, near1),
        2: jnp.where(up, near2, far2),
        -2: jnp.where(up, far2, near2),
        3: jnp.where(up, near3, zero),
        -3: jnp.where(up, zero, near3),
    }


def roll(x, shift, axis):
    n = x.shape[axis]
    shift = shift % n
    return x if shift == 0 else pltpu.roll(x, shift, axis)


def sweep_ring(q, u, axis):
    terms = remesh_terms(u, roll(u, 1, axis), roll(u, -1, axis), q)
    total = terms[0]
    for m in (1, -1, 2, -2, 3, -3):
        total = total + roll(terms[m], m, axis)
    return total


def swap_blocks(x):
    row = iota((8, 128), 0)
    block = iota((8, 128), 1) >> 4
    for bit in (1, 2, 4):
        low = (row & bit) == 0
        first = (block & bit) == 0
        upward = roll(roll(x, -bit, 0), 16 * bit, 1)
        downward = roll(roll(x, bit, 0), -16 * bit, 1)
        x = jnp.where(low == first, x, jnp.where(low, upward, downward))
    return x


def pack_velocity(v_ref, after_ref, out_ref):
    lane = iota((8, 128), 1)
    tiles = []
    for c in range(3):
        block = v_ref[c].reshape(128, 64) * (1.0 / 18.0)
        block = jnp.concatenate([block, jnp.zeros((128, 64), F32)], axis=1).T
        tiles.append([swap_blocks(block[8 * n : 8 * n + 8]) for n in range(8)])
    zero = jnp.zeros((8, 128), F32)
    for k in range(16):
        n, odd = divmod(k, 2)
        if odd == 0:
            out_ref[k, 0:8, :] = jnp.where(lane < 64, tiles[0][n], roll(tiles[1][n], 64, 1))
            before = tiles[2][n - 1] if n > 0 else zero
            planes = jnp.where(lane < 16, roll(before, 16, 1), roll(tiles[2][n], 16, 1))
        else:
            out_ref[k, 0:8, :] = jnp.where(lane < 64, roll(tiles[0][n], -64, 1), tiles[1][n])
            after = tiles[2][n + 1] if n < 7 else zero
            planes = jnp.where(lane < 80, roll(tiles[2][n], -48, 1), roll(after, 80, 1))
        out_ref[k, 8:16, :] = jnp.where(lane < 96, planes, zero)


def odd_device():
    return lax.axis_index("gz") & 1


def pack_chunks(s_ref, r_ref, out_ref, t_ref):
    flip = odd_device() * 3
    for v in range(6):
        part = slice(128 * v, 128 * v + 128)
        block = jnp.concatenate([s_ref[p ^ flip, :, part] for p in range(4)] + [jnp.zeros((32, 128), F32)], axis=0)
        t_ref[part, :] = block.T
    shape = (16, 8, 128)
    lane = iota(shape, 2)
    row = iota(shape, 1)
    col = lane & 15
    slot = lane >> 4

    def block(x, step):
        return jnp.concatenate([x[step:], x[:step]], axis=0)

    here, depth = r_ref[:, 0:8, :], r_ref[:, 8:16, :]
    wide = jnp.where(col == 0, block(roll(here, -15, 2), -1), roll(here, 1, 2))
    even = (wide, here, depth)
    wide = jnp.where(col < 9, roll(here, -7, 2), block(roll(here, 9, 2), 1))
    near = jnp.where(col < 8, roll(here, -8, 2), block(roll(here, 8, 2), 1))
    depth = jnp.where(col < 8, roll(depth, -8, 2), block(roll(depth, 8, 2), 1))
    stash = []
    for parity, (wide, near, depth) in enumerate((even, (wide, near, depth))):
        tile = jnp.where(slot < 4, wide, near)
        tile = jnp.where((slot >= 4) & (col >= 9), roll(depth, 73, 2), tile)
        tile = jnp.where((slot < 2) & (col >= 11), roll(depth, -53, 2), tile)
        tile = jnp.where(((slot >> 1) == 1) & (col >= 11), roll(depth, -26, 2), tile)
        rest = jnp.where((slot < 4) & ((col == 7) | (col == 8)), depth, 0.0)
        for bit in (1, 2, 4):
            rest = jnp.where((row & bit) == 0, roll(rest, -bit, 1), roll(rest, bit, 1))
        rest = jnp.stack([pltpu.roll(rest[n], 0, 1, stride=2, stride_axis=0) for n in range(16)])
        for bit in (4, 2, 1):
            rest = rest + roll(rest, bit, 1)
        stash.append(rest)
        for n in range(16):
            out_ref[2 * n + parity, 24:32, :] = tile[n]
    lane = iota((8, 128), 1)
    row = iota((8, 128), 0)
    for i in range(32):
        left = t_ref[(24 * i - 8) % 768 : (24 * i - 8) % 768 + 8, :]
        right = t_ref[(24 * i + 24) % 768 : (24 * i + 24) % 768 + 8, :]
        halo = jnp.where(row < 3, right, jnp.where(row == 3, stash[i % 2][i // 2], left))
        for t in range(3):
            tile = t_ref[24 * i + 8 * t : 24 * i + 8 * t + 8, :]
            out_ref[i, 8 * t : 8 * t + 8, :] = jnp.where(lane < 96, tile, roll(halo, 96 - 32 * t, 1))


def hat_rows(rows, slot, ring):
    e = iota((rows, 128), 0)
    if ring:
        e = jnp.where(e > 28, e - 32, e) + 3
    lane = iota((rows, 128), 1)
    away = jnp.abs(e - 3 * (lane & 15))
    return jnp.where((lane >> 4) == slot, jnp.maximum(3 - away, 0), 0)


def weights(y_ref, near_ref, near_z_ref, far_ref, far_z_ref):
    odd = odd_device()
    for v in range(6):
        c = iota((256, 128), 0)
        f = iota((256, 128), 1) + 128 * v
        away = jnp.abs(f - 3 * c)
        away = jnp.minimum(away, 768 - away)
        y_ref[:, 128 * v : 128 * v + 128] = jnp.maximum(3 - away, 0).astype(F32).astype(BF16)

    def both(rows):
        return jnp.concatenate(rows, axis=0).astype(F32).astype(BF16)

    sign = 1 - 2 * odd
    for planes, speeds, xy_ref, z_ref in (((0, 1, 2), range(5), near_ref, near_z_ref), ((3,), range(6), far_ref, far_z_ref)):
        xy = both([hat_rows(32, p ^ (3 * odd), True) for p in planes] + [hat_rows(24, 4 + (p ^ (3 * odd)), False) for p in planes])
        z = both([hat_rows(24, jnp.where(odd == 1, 5 - p, p), False) * sign for p in speeds])
        xy_ref[:, 0:128] = xy
        xy_ref[:, 128:256] = xy
        z_ref[:, 0:128] = z
        z_ref[:, 128:256] = z


def two_pieces(x):
    hi = x.astype(BF16)
    return jnp.concatenate([hi, (x - hi.astype(F32)).astype(BF16)], axis=0)


def unpack(s_ref, f_ref, c_ref, h_ref, planes):
    shape = (32, 8, 128)
    lane = iota(shape, 2)
    row = iota(shape, 1)
    col = lane & 15
    slot = lane >> 4
    parts = [roll(s_ref[:, 8 * t : 8 * t + 8, :], 32 * t - 96, 2) for t in range(3)]
    halo = jnp.where(lane < 32, parts[0], jnp.where(lane < 64, parts[1], parts[2]))
    h_ref[...] = halo
    packed = s_ref[:, 24:32, :]
    c_ref[0] = packed.reshape(256, 128)
    rest = jnp.broadcast_to(halo[:, 3:4, :], shape).reshape(256, 128)
    rest = jnp.stack([pltpu.roll(rest[8 * i : 8 * i + 8], 114, 1, stride=2, stride_axis=0) for i in range(32)])
    depth = jnp.where(slot >= 4, jnp.where(col < 5, roll(packed, 53, 2), roll(packed, 26, 2)), jnp.where(col < 7, roll(packed, -73, 2), rest))
    c_ref[1] = depth.reshape(256, 128)
    for i in range(32):
        whole = jnp.concatenate([s_ref[i, 0:24, :], h_ref[i]], axis=0)
        v, at = divmod(24 * i, 128)
        here = min(24, 128 - at)
        for n, p in enumerate(planes):
            moved = roll(whole, at - 24 * p, 1)
            f_ref[n, :, 128 * v + at : 128 * v + at + here] = moved[:, at : at + here]
            if here < 24:
                f_ref[n, :, 128 * v + 128 : 128 * v + 128 + 24 - here] = moved[:, : 24 - here]


def refine(coarse, y_ref, hats_ref, p_ref, out_ref):
    both = two_pieces(coarse.T)
    for n in range(3):
        part = slice(256 * n, 256 * n + 256)
        fine = jnp.dot(both, y_ref[:, part], preferred_element_type=F32)
        p_ref[:, part] = two_pieces(fine[:128] + fine[128:])
    for n in range(3):
        part = slice(256 * n, 256 * n + 256)
        out_ref[:, part] = jnp.dot(hats_ref[...], p_ref[:, part], preferred_element_type=F32)


def plane_sweeps(f_ref, u_ref, x_ref, q_ref, b_ref, count):
    def along_x(v, carry):
        part = pl.ds(pl.multiple_of(128 * v, 128), 128)
        for p in range(count):
            u = u_ref[32 * p : 32 * p + 32, part]
            terms = remesh_terms(u, roll(u, 1, 0), roll(u, -1, 0), f_ref[p, :, part])
            for n, m in enumerate((1, -1, 2, -2, 3, -3)):
                if m > 0:
                    b_ref[p, n, 0:8, :] = terms[m][24:32]
                    b_ref[p, n, 8:32, :] = terms[m][0:24]
                else:
                    b_ref[p, n, 8:40, :] = terms[m]
            total = terms[0][:24]
            for n, m in enumerate((1, -1, 2, -2, 3, -3)):
                total = total + b_ref[p, n, 8 - m : 32 - m, :]
            x_ref[p, :, part] = total
        return carry

    lax.fori_loop(0, 6, along_x, 0, unroll=True)

    def along_y(t, carry):
        for p in range(count):
            rows = pl.ds(pl.multiple_of(8 * t, 8), 8)
            speed = u_ref[pl.ds(pl.multiple_of(32 * count + 24 * p + 8 * t, 8), 8), :]
            q_ref[p, rows, :] = sweep_ring(x_ref[p, rows, :], speed, 1)
        return carry

    lax.fori_loop(0, 3, along_y, 0)


def near_planes(s_ref, y_ref, hats_ref, hats_z_ref, outer_ref, q_ref, f_ref, c_ref, h_ref, p_ref, u_ref, w_ref, x_ref, b_ref):
    unpack(s_ref, f_ref, c_ref, h_ref, (0, 1, 2))
    refine(c_ref[0], y_ref, hats_ref, p_ref, u_ref)
    refine(c_ref[1], y_ref, hats_z_ref, p_ref, w_ref)
    plane_sweeps(f_ref, u_ref, x_ref, q_ref, b_ref, 3)

    def along_z(v, carry):
        part = pl.ds(pl.multiple_of(128 * v, 128), 128)
        for t in range(3):
            rows = slice(8 * t, 8 * t + 8)
            speeds = [w_ref[24 * p + 8 * t : 24 * p + 8 * t + 8, part] for p in range(5)]
            first, second, third = [remesh_terms(speeds[p + 1], speeds[p], speeds[p + 2], q_ref[p, rows, part]) for p in range(3)]
            outer_ref[0, rows, part] = first[-1] + second[-2] + third[-3]
            outer_ref[1, rows, part] = first[-2] + second[-3]
            outer_ref[2, rows, part] = first[-3]
        return carry

    lax.fori_loop(0, 6, along_z, 0, unroll=True)


def far_plane(s_ref, y_ref, hats_ref, hats_z_ref, near_ref, own_ref, inner_ref, f_ref, c_ref, h_ref, p_ref, u_ref, w_ref, x_ref, b_ref, q_ref):
    unpack(s_ref, f_ref, c_ref, h_ref, (3,))
    refine(c_ref[0], y_ref, hats_ref, p_ref, u_ref)
    refine(c_ref[1], y_ref, hats_z_ref, p_ref, w_ref)
    plane_sweeps(f_ref, u_ref, x_ref, q_ref, b_ref, 1)

    def along_z(v, carry):
        part = pl.ds(pl.multiple_of(128 * v, 128), 128)
        for t in range(3):
            rows = slice(8 * t, 8 * t + 8)
            speeds = [w_ref[24 * p + 8 * t : 24 * p + 8 * t + 8, part] for p in range(6)]
            total = {}
            for p in range(4):
                q = q_ref[0, rows, part] if p == 3 else near_ref[p, rows, part]
                terms = remesh_terms(speeds[p + 1], speeds[p], speeds[p + 2], q)
                for m, term in terms.items():
                    total[p + m] = total[p + m] + term if p + m in total else term
            for n in range(4):
                own_ref[n, rows, part] = total[n]
            for n in range(3):
                inner_ref[n, rows, part] = total[4 + n]
        return carry

    lax.fori_loop(0, 6, along_z, 0, unroll=True)


def join(own_ref, outer_ref, inner_ref, out_ref):
    flip = odd_device() * 3
    scale = 1.0 / 27.0
    out_ref[0 ^ flip] = (own_ref[0] + outer_ref[0]) * scale
    out_ref[1 ^ flip] = (own_ref[1] + outer_ref[1] + inner_ref[2]) * scale
    out_ref[2 ^ flip] = (own_ref[2] + outer_ref[2] + inner_ref[1]) * scale
    out_ref[3 ^ flip] = (own_ref[3] + inner_ref[0]) * scale


def kernel(body, *shapes, scratch=(), flops=1e7, specs=None):
    outs = tuple(jax.ShapeDtypeStruct(*(s if isinstance(s[0], tuple) else (s, F32))) for s in shapes)
    extra = {"in_specs": [pl.BlockSpec(memory_space=m) for m in specs]} if specs else {}
    return pl.pallas_call(
        body,
        out_shape=outs if len(outs) > 1 else outs[0],
        scratch_shapes=[pltpu.VMEM(*(s if isinstance(s[0], tuple) else (s, F32))) for s in scratch],
        cost_estimate=pl.CostEstimate(flops=int(flops), transcendentals=0, bytes_accessed=1 << 20),
        compiler_params=pltpu.CompilerParams(vmem_limit_bytes=16 * 1024 * 1024),
        **extra,
    )


def exchange(x, axis):
    return lax.all_to_all(x, axis, split_axis=0, concat_axis=0, tiled=False)


def sweep_scratch(count, speeds):
    return [(count, 32, 768), (2, 256, 128), (32, 8, 128), ((256, 768), BF16), (56 * count, 768), (24 * speeds, 768), (count, 24, 768), (count, 6, 40, 128)]


def steps(scalar, velocity):
    tables = [(t, BF16) for t in ((256, 768), (168, 256), (120, 256), (56, 256), (144, 256))]
    y_weights, near, near_z, far, far_z = kernel(weights, *tables, flops=1e9)()
    coarse = jnp.transpose(velocity, (0, 2, 3, 1))
    planes = exchange(kernel(pack_velocity, (16, 16, 128), specs=(pltpu.VMEM, pl.ANY))(coarse, near), "gz")
    chunks = exchange(kernel(pack_chunks, (32, 32, 128), scratch=[(768, 128)])(scalar, planes), "gy")
    outer, swept = kernel(near_planes, (3, 24, 768), (3, 24, 768), scratch=sweep_scratch(3, 5))(chunks, y_weights, near, near_z)
    count = lax.axis_size("gz")
    pairs = [(k, k + 1) for k in range(1, count - 1, 2)]
    outer = lax.ppermute(outer, "gz", pairs + [(b, a) for a, b in pairs])
    own, inner = kernel(far_plane, (4, 24, 768), (3, 24, 768), scratch=sweep_scratch(1, 6) + [(1, 24, 768)], flops=1e9)(chunks, y_weights, far, far_z, swept)
    pairs = [(k, k + 1) for k in range(0, count, 2)]
    inner = lax.ppermute(inner, "gz", pairs + [(b, a) for a, b in pairs])
    return kernel(join, (4, 24, 768))(own, outer, inner)


def solution(mesh):
    in_specs = (P("gz", "gy", None), P(None, None, "gy", "gz"))
    out_specs = P("gz", "gy", None)
    return jax.shard_map(steps, mesh=mesh, in_specs=in_specs, out_specs=out_specs, check_vma=False)
```
